32 devices in a mesh: groups: 1, section: 2 (over x), axial: 16 (over z, y, core).
Axes of the slice: x: 2, y: 2, z: 4, core: 2. Of those that a mesh axis runs over, the one named last changes fastest.
Arguments:
- pair_in: bfloat16 [4, 128, 128, 128], P('groups', 'axial'), may hold values from -6 to 6
- crop_mask: int32 [4, 128], P('groups'), may hold values 0 or 1
- proj_weights: bfloat16 [2, 5, 128, 128], P('section'), may hold values from -0.5 to 0.5
- out_weights: bfloat16 [2, 128, 128], P('section'), may hold values from -0.5 to 0.5
- up_weights: bfloat16 [2, 128, 512], P('section'), may hold values from -0.5 to 0.5
- down_weights: bfloat16 [2, 512, 128], P('section'), may hold values from -0.25 to 0.25
- norm_gains: bfloat16 [2, 3, 128], P('section'), may hold values from 0.099609375 to 1.8984375
Outputs:
- pair_out: bfloat16 [4, 128, 128, 128], P(('groups', 'section'), 'axial')
The draws below stay inside these ranges and needn't reach their ends.
Inputs may be any that keep to these rules, and one draw needn't show every extreme that they name: `crop_mask`: 1 marks a residue inside the crop, 0 a padded one.
All inputs are finite; a program needn't handle non-finite values.
Results may differ from the reference program's by a relative error of at most 0.013.
Values may be sent and summed in bfloat16 or wider, within the bound.
A program may use at most 64 MiB of HBM per device.

```python
import jax
import jax.numpy as jnp
from jax import lax

C = 128
MB = 4
N = 128
BLOCKS = 2
FF = 512


def touch_ends(entries, key, smallest, high):
    extent = entries.shape
    place = [jax.random.randint(jax.random.fold_in(key, axis), (), 0, extent[axis]) for axis in range(len(extent))]
    entries = entries.at[tuple(place)].set(smallest)
    longest = extent.index(max(extent))
    place[longest] = (place[longest] + 1) % extent[longest]
    return entries.at[tuple(place)].set(high)


def shard_levels(key, extent, shards, smallest, largest):
    loudness = 1.0
    for axis_at, blocks in shards:
        steps = jax.random.uniform(jax.random.fold_in(jax.random.fold_in(key, 6), axis_at), (blocks,), jnp.float32, smallest / len(shards), largest / len(shards))
        loudness = loudness * jnp.repeat(jnp.exp(steps), extent[axis_at] // blocks).reshape((-1,) + (1,) * (len(extent) - 1 - axis_at))
    return loudness


def scatter_about(stream_key, dims, scale, reach, split=(), dtype=jnp.bfloat16):
    level = shard_levels(stream_key, dims, split, -0.22, 0.18) if split else 1.0
    drawn = jax.random.normal(stream_key, dims, jnp.float32) * scale * level
    return jnp.minimum(jnp.maximum(drawn, -reach), reach).astype(dtype)


def setup_inputs(seed: int = 0, part: int = 0) -> dict:
    splits = jax.random.split(jax.random.key(seed), 8)
    part_splits = jax.random.split(jax.random.fold_in(splits[7], part), 8)
    pair_in = scatter_about(part_splits[0], (MB, N, N, C), 1.0, 6.0, ((1, 16),))
    crop_mask = touch_ends((jax.random.randint(part_splits[1], (MB, N), 0, 8) < 7).astype(jnp.int32), jax.random.fold_in(part_splits[1], 1), 0, 1)
    proj_weights = scatter_about(splits[2], (BLOCKS, 5, C, C), C ** -0.5, 0.5, ((0, 2),))
    out_weights = scatter_about(splits[3], (BLOCKS, C, C), C ** -0.5, 0.5, ((0, 2),))
    up_weights = scatter_about(splits[4], (BLOCKS, C, FF), C ** -0.5, 0.5, ((0, 2),))
    down_weights = scatter_about(splits[5], (BLOCKS, FF, C), FF ** -0.5, 0.25, ((0, 2),))
    norm_gains = jnp.clip(1.0 + 0.18 * jax.random.normal(splits[6], (BLOCKS, 3, C), jnp.float32), 0.099609375, 1.8984375).astype(jnp.bfloat16)
    return dict(pair_in=pair_in, crop_mask=crop_mask, proj_weights=proj_weights, out_weights=out_weights, up_weights=up_weights, down_weights=down_weights, norm_gains=norm_gains)


epsilon = 1e-05

def normalize(values, axis_dim):
    center = values - lax.optimization_barrier(jnp.mean(values, axis=axis_dim, keepdims=True))
    spread = lax.optimization_barrier(jnp.mean(center * center, axis=axis_dim, keepdims=True))
    return center * lax.rsqrt(spread + epsilon)

def evo_block(current, mask_all, proj_mats, out_mat, up_mat, down_mat, gain_rows):
    channels = current.shape[2]
    gain_vals = gain_rows.astype(jnp.float32)
    pair_f = current.astype(jnp.float32)
    normed = (normalize(pair_f, 2) * gain_vals[0]).astype(jnp.bfloat16)
    linear = jnp.einsum('ijd,edc->ecij', normed.astype(jnp.float32), proj_mats[:4].astype(jnp.float32))
    pair_mask = mask_all[:, None] * mask_all[None, :]
    left_edge = (jax.nn.sigmoid(linear[1]) * linear[0] * pair_mask).astype(jnp.bfloat16)
    right_edge = (jax.nn.sigmoid(linear[3]) * linear[2] * pair_mask).astype(jnp.bfloat16)
    product = jnp.einsum('cik,cjk->cij', left_edge.astype(jnp.float32), right_edge.astype(jnp.float32)).astype(jnp.bfloat16)
    tri_norm = (normalize(product.astype(jnp.float32), 0) * gain_vals[1][:, None, None]).astype(jnp.bfloat16)
    update = jnp.einsum('cij,cd->ijd', tri_norm.astype(jnp.float32), out_mat.astype(jnp.float32))
    gate_values = jax.nn.sigmoid(jnp.einsum('ijd,dc->ijc', normed.astype(jnp.float32), proj_mats[4].astype(jnp.float32)))
    pair_mid = pair_f + gate_values * update
    trans_in = (normalize(pair_mid, 2) * gain_vals[2]).astype(jnp.bfloat16).reshape(-1, channels)
    hidden = jax.nn.relu(jnp.dot(trans_in, up_mat, preferred_element_type=jnp.float32)).astype(jnp.bfloat16)
    pair_new = pair_mid + jnp.dot(hidden, down_mat, preferred_element_type=jnp.float32).reshape(pair_mid.shape)
    return pair_new.astype(jnp.bfloat16)

def reference(pair_in, crop_mask, proj_weights, out_weights, up_weights, down_weights, norm_gains):
    finished = []
    for micro_index in range(MB):
        current = pair_in[micro_index]
        mask_all = crop_mask[micro_index].astype(jnp.float32)
        for layer_index in range(BLOCKS):
            current = evo_block(current, mask_all, proj_weights[layer_index], out_weights[layer_index], up_weights[layer_index], down_weights[layer_index], norm_gains[layer_index])
        finished.append(current)
    return jnp.stack(finished)
```

```python
import functools

import jax
import jax.numpy as jnp
from jax import lax
from jax.experimental import pallas as pl
from jax.experimental.pallas import tpu as pltpu
from jax.sharding import PartitionSpec as P

epsilon = 1e-05


def normalize(values, axis_dim):
    center = values - jnp.mean(values, axis=axis_dim, keepdims=True)
    spread = jnp.mean(center * center, axis=axis_dim, keepdims=True)
    return center * lax.rsqrt(spread + epsilon)


def triangle(pieces):
    return jnp.einsum(
        "gcik,gcjk->gcij", pieces[0], pieces[1], preferred_element_type=jnp.float32
    ).astype(jnp.bfloat16)


def evo_block(current, mask_all, proj_mats, out_mat, up_mat, down_mat, gain_rows):
    row_count = current.shape[0]
    width = current.shape[1]
    channels = current.shape[2]
    group_count = lax.axis_size("axial")
    per_group = channels // group_count
    row_start = lax.axis_index("axial") * row_count
    mask_rows = lax.dynamic_slice_in_dim(mask_all, row_start, row_count)
    gain_vals = gain_rows.astype(jnp.float32)
    pair_f = current.astype(jnp.float32)
    normed = (normalize(pair_f, 2) * gain_vals[0]).astype(jnp.bfloat16)
    linear = jnp.einsum("rnd,edc->ecrn", normed, proj_mats[:4], preferred_element_type=jnp.float32)
    pair_mask = mask_rows[:, None] * mask_all[None, :]
    left_edge = (jax.nn.sigmoid(linear[1]) * linear[0] * pair_mask).astype(jnp.bfloat16)
    right_edge = (jax.nn.sigmoid(linear[3]) * linear[2] * pair_mask).astype(jnp.bfloat16)
    left_groups = left_edge.reshape(group_count, per_group, row_count, width)
    right_groups = right_edge.reshape(group_count, per_group, row_count, width)
    product = triangle(
        (
            lax.all_to_all(left_groups, "axial", split_axis=0, concat_axis=2, tiled=True),
            lax.all_to_all(right_groups, "axial", split_axis=0, concat_axis=2, tiled=True),
        )
    )
    restored = lax.all_to_all(product, "axial", split_axis=2, concat_axis=0, tiled=True).reshape(
        channels, row_count, width
    )
    tri_norm = (normalize(restored.astype(jnp.float32), 0) * gain_vals[1][:, None, None]).astype(
        jnp.bfloat16
    )
    update = jnp.einsum("crn,cd->rnd", tri_norm, out_mat, preferred_element_type=jnp.float32)
    gate_values = jax.nn.sigmoid(
        jnp.einsum("rnd,dc->rnc", normed, proj_mats[4], preferred_element_type=jnp.float32)
    )
    pair_mid = pair_f + gate_values * update
    trans_in = (normalize(pair_mid, 2) * gain_vals[2]).astype(jnp.bfloat16).reshape(-1, channels)
    hidden = jax.nn.relu(jnp.dot(trans_in, up_mat, preferred_element_type=jnp.float32)).astype(
        jnp.bfloat16
    )
    pair_new = pair_mid + jnp.dot(hidden, down_mat, preferred_element_type=jnp.float32).reshape(
        pair_mid.shape
    )
    return pair_new.astype(jnp.bfloat16)


MESH = pl.DeviceIdType.MESH


def sigmoid(values):
    return 0.5 * jnp.tanh(0.5 * values) + 0.5


def normalize_rows(values, gain):
    scale = 1.0 / values.shape[0]
    center = values - jnp.sum(values, axis=0, keepdims=True) * scale
    spread = jnp.sum(center * center, axis=0, keepdims=True) * scale
    return center * lax.rsqrt(spread + epsilon) * gain


def matmul(mat, values):
    return lax.dot_general(mat, values, (((1,), (0,)), ((), ())), preferred_element_type=jnp.float32)


def fused_kernel(
    sections,
    ranks,
    halves,
    own_count,
    sub_rows,
    pair_ref,
    mask_ref,
    mask_smem,
    proj_ref,
    out_ref,
    up_ref,
    down_ref,
    gain_ref,
    result_ref,
    pair_buf,
    z_buf,
    normed_buf,
    gate_buf,
    edge_send,
    edge_recv,
    tri_send,
    tri_recv,
    left_f,
    right_f,
    tri_f,
    result_buf,
    proj_raw,
    out_raw,
    up_raw,
    down_raw,
    gain_all,
    proj_t,
    out_t,
    up_t,
    down_t,
    gain_t,
    pair_send_sem,
    pair_sem,
    edge_send_sem,
    edge_recv_sem,
    tri_send_sem,
    tri_recv_sem,
    result_send_sem,
    result_recv_sem,
    raw_sem,
    weight_send_sem,
    weight_pass_sem,
    weight_sem,
):
    section = lax.axis_index("section")
    axial = lax.axis_index("axial")
    span = ranks // sections
    group = axial // span
    place = lax.rem(axial, span)
    core = lax.rem(axial, 2)
    rank = section * span + place
    piece_rows, width, channels = pair_buf.shape[2:]
    rows = piece_rows * sections
    owners = ranks // halves
    per_group = channels // owners
    my_half = rank // owners
    my_owner = lax.rem(rank, owners)
    steps = piece_rows // sub_rows
    everyone = range(own_count)
    pieces = range(sections)

    def member(index):
        return {"section": index // span, "axial": group * span + lax.rem(index, span)}

    def part_of(t):
        return lax.rem(group + t, sections)

    def first_row(t, section_at, place_at):
        return (part_of(t) * span + place_at) * rows + section_at * piece_rows

    own_rows = pl.ds(section * piece_rows, piece_rows)

    for m in everyone:
        pltpu.make_async_copy(
            pair_ref.at[group * own_count + m, own_rows], pair_buf.at[m, 0], pair_sem.at[m, 0]
        ).start()
    raw_copies = [
        pltpu.make_async_copy(source, target, raw_sem.at[index])
        for index, (source, target) in enumerate(
            (
                (gain_ref.at[0], gain_all.at[section]),
                (proj_ref.at[0, pl.ds(2, 2)], proj_raw.at[pl.ds(2, 2)]),
                (proj_ref.at[0, pl.ds(0, 2)], proj_raw.at[pl.ds(0, 2)]),
                (proj_ref.at[0, pl.ds(4, 1)], proj_raw.at[pl.ds(4, 1)]),
                (out_ref.at[0], out_raw),
                (up_ref.at[0], up_raw),
                (down_ref.at[0], down_raw),
            )
        )
    ]
    for copy in raw_copies:
        copy.start()

    barrier = pltpu.get_barrier_semaphore()
    for k in range(1, ranks):
        pl.semaphore_signal(
            barrier, inc=1, device_id=member(lax.rem(rank + k, ranks)), device_id_type=MESH
        )
    for k in range(1, sections):
        for j in range(sections):
            pl.semaphore_signal(
                barrier,
                inc=1,
                device_id={
                    "section": lax.rem(section + j, sections),
                    "axial": part_of(k) * span + place,
                },
                device_id_type=MESH,
            )

    items = (
        (0, lambda layer: gain_all.at[layer]),
        (0, lambda layer: proj_t.at[layer, 2]),
        (1, lambda layer: proj_t.at[layer, 3]),
        (0, lambda layer: proj_t.at[layer, 0]),
        (1, lambda layer: proj_t.at[layer, 1]),
        (0, lambda layer: proj_t.at[layer, 4]),
        (1, lambda layer: out_t.at[layer]),
        (0, lambda layer: up_t.at[layer]),
        (1, lambda layer: down_t.at[layer]),
    )

    def item_copy(a, k):
        view = items[a][1](section)
        return pltpu.make_async_remote_copy(
            src_ref=view,
            dst_ref=view,
            send_sem=weight_send_sem.at[a, k],
            recv_sem=weight_sem.at[a, section],
            device_id={"section": lax.rem(section + k, sections)},
            device_id_type=MESH,
        )

    def item_pass(a, layer):
        view = items[a][1](layer)
        return pltpu.make_async_remote_copy(
            src_ref=view,
            dst_ref=view,
            send_sem=weight_pass_sem.at[a, layer],
            recv_sem=weight_sem.at[a, layer],
            device_id={"axial": axial + 1 - 2 * core},
            device_id_type=MESH,
        )

    def send_items(chosen):
        for side in range(2):

            @pl.when(core == side)
            def start():
                for a in chosen:
                    if items[a][0] == side:
                        for k in range(1, sections):
                            item_copy(a, k).start()

    def take_items(chosen, layer):
        for a in chosen:
            view = items[a][1](layer)
            pltpu.make_async_copy(view, view, weight_sem.at[a, layer]).wait()

            @pl.when(core == items[a][0])
            def pass_on():
                item_pass(a, layer).start()

    def finish_items():
        for side in range(2):

            @pl.when(core == side)
            def finish():
                for a, (owner, _) in enumerate(items):
                    if owner == side:
                        for k in range(1, sections):
                            item_copy(a, k).wait_send()
                        for k in range(1, sections):
                            item_pass(a, lax.rem(section + k, sections)).wait_send()

    def turned(values):
        return values.astype(jnp.float32).T.astype(jnp.bfloat16)

    def prepare_gains(layer):
        for index in range(gain_t.shape[1]):
            row = gain_all[layer, index : index + 1, :].astype(jnp.float32)
            gain_t[layer, index] = jnp.broadcast_to(row, (width, channels)).T

    def prepare_edges():
        raw_copies[0].wait()
        for pair in (1, 0):
            raw_copies[2 - pair].wait()
            for e in (2 * pair, 2 * pair + 1):
                proj_t[section, e] = turned(proj_raw[e])

    def prepare_rest():
        raw_copies[3].wait()
        proj_t[section, 4] = turned(proj_raw[4])
        for copy in raw_copies[4:]:
            copy.wait()
        out_t[section] = turned(out_raw[...])
        up_t[section] = turned(up_raw[...])
        down_t[section] = turned(down_raw[...])

    def wide_gain(layer, index):
        return jnp.concatenate([gain_t[layer, index]] * sub_rows, axis=1)

    def pair_copy(m, k):
        target = part_of(k)
        return pltpu.make_async_remote_copy(
            src_ref=pair_ref.at[target * own_count + m, own_rows],
            dst_ref=pair_buf.at[m, sections - k],
            send_sem=pair_send_sem.at[m, k],
            recv_sem=pair_sem.at[m, sections - k],
            device_id={"axial": target * span + place},
            device_id_type=MESH,
        )

    def load_pair(m, t):
        pltpu.make_async_copy(pair_buf.at[m, t], pair_buf.at[m, t], pair_sem.at[m, t]).wait()
        for q in range(steps):
            for i in range(sub_rows):
                z_buf[m, t, q, :, i * width : (i + 1) * width] = (
                    pair_buf[m, t, q * sub_rows + i].astype(jnp.float32).T
                )

    def phase_norm(layer, m, t):
        for q in range(steps):
            normed_buf[m, t, q] = normalize_rows(z_buf[m, t, q], wide_gain(layer, 0)).astype(
                jnp.bfloat16
            )

    def phase_edges(layer, m, t):
        crop = group * own_count + m
        row_mask = mask_ref[pl.ds(crop, 1), :].astype(jnp.float32)
        start = first_row(t, section, place)
        for q in range(steps):
            values = normed_buf[m, t, q]
            masks = []
            for i in range(sub_rows):
                own = mask_smem[crop, start + q * sub_rows + i]
                masks.append(row_mask * own.astype(jnp.float32))
            pair_mask = jnp.concatenate(masks, axis=1)
            for side in (1, 0):
                value = matmul(proj_t[layer, 2 * side], values)
                gate = matmul(proj_t[layer, 2 * side + 1], values)
                edge = sigmoid(gate) * value * pair_mask
                for i in range(sub_rows):
                    part = edge[:, i * width : (i + 1) * width].reshape(owners, per_group, width)
                    edge_send[m, t, :, side, q * sub_rows + i] = part.astype(jnp.bfloat16)

    def phase_gate(layer, m, t):
        for q in range(steps):
            gate_buf[m, t, q] = sigmoid(matmul(proj_t[layer, 4], normed_buf[m, t, q]))

    def rank_at(half_step, index):
        if halves == 1:
            return index
        return lax.rem(my_half + half_step, halves) * owners + index

    def edge_view(ref, half_step):
        return ref if half_step == 0 else ref.at[1]

    def edge_copy(slot, m, t, k):
        half_step = k // owners
        owner = lax.rem(my_owner + k % owners, owners)
        return pltpu.make_async_remote_copy(
            src_ref=edge_view(edge_send.at[m, t, owner], half_step),
            dst_ref=edge_view(edge_recv.at[slot, m, t, rank], half_step),
            send_sem=edge_send_sem.at[m, t, k],
            recv_sem=edge_recv_sem.at[slot, m, t, rank],
            device_id=member(rank_at(half_step, owner)),
            device_id_type=MESH,
        )

    def send_edges(slot, m, t):
        for k in range(ranks - 1, 0, -1):
            edge_copy(slot, m, t, k).start()
        pltpu.make_async_copy(
            edge_send.at[m, t, my_owner],
            edge_recv.at[slot, m, t, rank],
            edge_recv_sem.at[slot, m, t, rank],
        ).start()

    def wait_edges_sent(slot, m, t):
        for k in range(1, ranks):
            edge_copy(slot, m, t, k).wait_send()

    def tri_copy(m, k):
        owner = lax.rem(my_owner + k, owners)
        return pltpu.make_async_remote_copy(
            src_ref=tri_send.at[m, owner],
            dst_ref=tri_recv.at[m, my_owner],
            send_sem=tri_send_sem.at[m, k],
            recv_sem=tri_recv_sem.at[m, my_owner],
            device_id=member(my_half * owners + owner),
            device_id_type=MESH,
        )

    def send_tri(m):
        for k in range(owners - 1, 0, -1):
            tri_copy(m, k).start()
        pltpu.make_async_copy(
            tri_send.at[m, my_owner], tri_recv.at[m, my_owner], tri_recv_sem.at[m, my_owner]
        ).start()

    def wait_tri_sent(m):
        for k in range(1, owners):
            tri_copy(m, k).wait_send()

    def wait_tri(m):
        for g in range(owners):
            pltpu.make_async_copy(tri_recv.at[m, g], tri_recv.at[m, g], tri_recv_sem.at[m, g]).wait()

    def phase_triangle(slot, m):
        for t in pieces:
            for half_step in range(halves):
                for index in range(owners):
                    g = rank_at(half_step, index)
                    whole = edge_view(edge_recv.at[slot, m, t, g], half_step)
                    pltpu.make_async_copy(whole, whole, edge_recv_sem.at[slot, m, t, g]).wait()
                    start = first_row(t, g // span, g % span if halves == 1 else lax.rem(g, span))
                    right_f[pl.ds(start, piece_rows)] = edge_recv[slot, m, t, g, 1].astype(
                        jnp.float32
                    )
                    if half_step == 0:
                        at = index * rows + t * piece_rows
                        left_f[at : at + piece_rows] = edge_recv[slot, m, t, g, 0].astype(
                            jnp.float32
                        )
        for c in range(per_group):
            tri_f[:, c, :] = lax.dot_general(
                left_f[:, c, :].astype(jnp.bfloat16),
                right_f[:, c, :].astype(jnp.bfloat16),
                (((1,), (1,)), ((), ())),
                preferred_element_type=jnp.float32,
            )
        for g in range(owners):
            tri_send[m, g] = tri_f[g * rows : (g + 1) * rows].astype(jnp.bfloat16)

    def phase_update(layer, m, t, last):
        for q in range(steps):
            parts = []
            for i in range(sub_rows):
                part = tri_recv[m, :, t * piece_rows + q * sub_rows + i].astype(jnp.float32)
                parts.append(part.reshape(channels, width))
            tri = jnp.concatenate(parts, axis=1)
            tri_norm = normalize_rows(tri, wide_gain(layer, 1)).astype(jnp.bfloat16)
            mid = z_buf[m, t, q] + gate_buf[m, t, q] * matmul(out_t[layer], tri_norm)
            trans_in = normalize_rows(mid, wide_gain(layer, 2)).astype(jnp.bfloat16)
            hidden = jnp.maximum(matmul(up_t[layer], trans_in), 0.0).astype(jnp.bfloat16)
            fresh = mid + matmul(down_t[layer], hidden)
            if last:
                for i in range(sub_rows):
                    part = fresh[:, i * width : (i + 1) * width]
                    result_buf[m, t, q * sub_rows + i] = part.T.astype(jnp.bfloat16)
            else:
                z_buf[m, t, q] = fresh.astype(jnp.bfloat16).astype(jnp.float32)

    def result_copy(m, t):
        return pltpu.make_async_remote_copy(
            src_ref=result_buf.at[m, t],
            dst_ref=result_ref.at[m, own_rows],
            send_sem=result_send_sem.at[m, t],
            recv_sem=result_recv_sem.at[m, section],
            device_id={"section": group, "axial": part_of(t) * span + place},
            device_id_type=MESH,
        )

    def send_result(m, t):
        if t > 0:
            result_copy(m, t).start()
            return

        @pl.when(section == group)
        def keep():
            pltpu.make_async_copy(
                result_buf.at[m, t], result_ref.at[m, own_rows], result_recv_sem.at[m, section]
            ).start()

        @pl.when(section != group)
        def give():
            result_copy(m, t).start()

    def finish_results():
        for m in everyone:
            for t in pieces:
                if t > 0:
                    result_copy(m, t).wait_send()
                else:

                    @pl.when(section != group)
                    def given():
                        result_copy(m, t).wait_send()

            for s in range(sections):
                part = result_ref.at[m, pl.ds(s * piece_rows, piece_rows)]
                pltpu.make_async_copy(part, part, result_recv_sem.at[m, s]).wait()

    edge_items = range(5)
    rest_items = range(5, len(items))
    prepare_edges()
    pl.semaphore_wait(barrier, ranks - 1 + (sections - 1) * sections)
    send_items(edge_items)
    for m in everyone:
        for k in range(1, sections):
            pair_copy(m, k).start()
    prepare_gains(section)
    for m in everyone:
        load_pair(m, 0)
    prepare_rest()
    send_items(rest_items)

    @pl.when(section != 0)
    def first_weights():
        take_items(edge_items, 0)
        prepare_gains(0)

    for t in pieces:
        for m in everyone:
            if t > 0:
                load_pair(m, t)
            phase_norm(0, m, t)
            phase_edges(0, m, t)
            send_edges(0, m, t)

    @pl.when(section != 0)
    def other_weights():
        take_items(rest_items, 0)

    for layer in range(1, sections):

        @pl.when(section != layer)
        def later_weights():
            take_items(range(len(items)), layer)
            prepare_gains(layer)

    for m in everyone:
        for t in pieces:
            phase_gate(0, m, t)

    for layer in range(sections):
        last = layer == sections - 1
        for m in everyone:
            if layer > 0:
                wait_tri_sent(m)
            phase_triangle(layer % 2, m)
            send_tri(m)
        for m in everyone:
            wait_tri(m)
            for t in pieces:
                phase_update(layer, m, t, last)
                wait_edges_sent(layer % 2, m, t)
                if last:
                    send_result(m, t)
                else:
                    phase_norm(layer + 1, m, t)
                    phase_edges(layer + 1, m, t)
                    send_edges((layer + 1) % 2, m, t)
        if not last:
            for m in everyone:
                for t in pieces:
                    phase_gate(layer + 1, m, t)
    for m in everyone:
        wait_tri_sent(m)
        for k in range(1, sections):
            pair_copy(m, k).wait_send()
    finish_items()
    finish_results()


def fused_device(pair_in, crop_mask, proj_weights, out_weights, up_weights, down_weights, norm_gains):
    sections = lax.axis_size("section")
    ranks = lax.axis_size("axial")
    micro_count, rows, width, channels = pair_in.shape
    own_count = micro_count // sections
    halves = half_count(pair_in)
    owners = ranks // halves
    per_group = channels // owners
    piece_rows = rows // sections
    sub_rows = 2 if piece_rows % 2 == 0 else 1
    steps = piece_rows // sub_rows
    lanes = sub_rows * width
    hidden = up_weights.shape[2]
    gains = norm_gains.shape[1]
    edge_kinds = proj_weights.shape[1]
    bf16, f32 = jnp.bfloat16, jnp.float32
    vmem = pl.BlockSpec(memory_space=pltpu.VMEM)
    hbm = pl.BlockSpec(memory_space=pltpu.HBM)
    dma = pltpu.SemaphoreType.DMA
    piece = (piece_rows, per_group, width)
    rows_shape = (own_count, sections, piece_rows, width, channels)
    wide_shape = (own_count, sections, steps, channels, lanes)
    tri_shape = (own_count, owners, rows, per_group, width)
    return pl.pallas_call(
        functools.partial(fused_kernel, sections, ranks, halves, own_count, sub_rows),
        out_shape=jax.ShapeDtypeStruct((own_count, rows, width, channels), bf16),
        in_specs=[hbm, vmem, pl.BlockSpec(memory_space=pltpu.SMEM)] + [hbm] * 5,
        out_specs=hbm,
        scratch_shapes=[
            pltpu.VMEM(rows_shape, bf16),
            pltpu.VMEM(wide_shape, f32),
            pltpu.VMEM(wide_shape, bf16),
            pltpu.VMEM(wide_shape, f32),
            pltpu.VMEM((own_count, sections, owners, 2) + piece, bf16),
            pltpu.VMEM((2, own_count, sections, ranks, 2) + piece, bf16),
            pltpu.VMEM(tri_shape, bf16),
            pltpu.VMEM(tri_shape, bf16),
            pltpu.VMEM((owners * rows, per_group, width), f32),
            pltpu.VMEM((ranks * rows, per_group, width), f32),
            pltpu.VMEM((owners * rows, per_group, width), f32),
            pltpu.VMEM(rows_shape, bf16),
            pltpu.VMEM(proj_weights.shape[1:], bf16),
            pltpu.VMEM(out_weights.shape[1:], bf16),
            pltpu.VMEM(up_weights.shape[1:], bf16),
            pltpu.VMEM(down_weights.shape[1:], bf16),
            pltpu.VMEM((sections,) + norm_gains.shape[1:], bf16),
            pltpu.VMEM((sections, edge_kinds, channels, channels), bf16),
            pltpu.VMEM((sections, channels, channels), bf16),
            pltpu.VMEM((sections, hidden, channels), bf16),
            pltpu.VMEM((sections, channels, hidden), bf16),
            pltpu.VMEM((sections, gains, channels, width), f32),
            dma((own_count, sections)),
            dma((own_count, sections)),
            dma((own_count, sections, ranks)),
            dma((2, own_count, sections, ranks)),
            dma((own_count, owners)),
            dma((own_count, owners)),
            dma((own_count, sections)),
            dma((own_count, sections)),
            dma((7,)),
            dma((9, sections)),
            dma((9, sections)),
            dma((9, sections)),
        ],
        compiler_params=pltpu.CompilerParams(
            collective_id=0, has_side_effects=True, vmem_limit_bytes=67043328
        ),
    )(
        pair_in,
        crop_mask,
        crop_mask,
        proj_weights,
        out_weights,
        up_weights,
        down_weights,
        norm_gains,
    )


def half_count(pair_in):
    ranks = lax.axis_size("axial")
    return 2 if ranks % 2 == 0 and pair_in.shape[3] % (8 * ranks) else 1


def fits_fused(pair_in):
    rows, width, channels = pair_in.shape[1:]
    sections = lax.axis_size("section")
    ranks = lax.axis_size("axial")
    owners = ranks // half_count(pair_in)
    return (
        channels % (8 * owners) == 0
        and rows % sections == 0
        and width % 128 == 0
        and ranks % (2 * sections) == 0
    )


def per_device(pair_in, crop_mask, proj_weights, out_weights, up_weights, down_weights, norm_gains):
    if fits_fused(pair_in):
        return fused_device(
            pair_in, crop_mask, proj_weights, out_weights, up_weights, down_weights, norm_gains
        )
    section_index = lax.axis_index("section")
    section_count = lax.axis_size("section")
    micro_count = pair_in.shape[0]
    own_count = micro_count // section_count
    gathered = (
        lax.all_gather(proj_weights, "section", axis=0, tiled=True),
        lax.all_gather(out_weights, "section", axis=0, tiled=True),
        lax.all_gather(up_weights, "section", axis=0, tiled=True),
        lax.all_gather(down_weights, "section", axis=0, tiled=True),
        lax.all_gather(norm_gains, "section", axis=0, tiled=True),
    )
    own_pairs = lax.dynamic_slice_in_dim(pair_in, section_index * own_count, own_count, 0)
    own_masks = lax.dynamic_slice_in_dim(crop_mask, section_index * own_count, own_count, 0).astype(
        jnp.float32
    )
    outputs = []
    for member in range(own_count):
        current = own_pairs[member]
        for layer_index in range(section_count):
            current = evo_block(
                current,
                own_masks[member],
                gathered[0][layer_index],
                gathered[1][layer_index],
                gathered[2][layer_index],
                gathered[3][layer_index],
                gathered[4][layer_index],
            )
        outputs.append(current)
    return jnp.stack(outputs)


def solution(mesh):
    return jax.shard_map(
        per_device,
        mesh=mesh,
        in_specs=(
            P("groups", "axial", None, None),
            P("groups", None),
            P("section", None, None, None),
            P("section", None, None),
            P("section", None, None),
            P("section", None, None),
            P("section", None, None),
        ),
        out_specs=P(("groups", "section"), "axial", None, None),
        check_vma=False,
    )
```

```python
import functools

import jax
import jax.numpy as jnp
from jax import lax
from jax.experimental import pallas as pl
from jax.experimental.pallas import tpu as pltpu
from jax.sharding import PartitionSpec as P

epsilon = 1e-05


def normalize(values, axis_dim):
    center = values - jnp.mean(values, axis=axis_dim, keepdims=True)
    spread = jnp.mean(center * center, axis=axis_dim, keepdims=True)
    return center * lax.rsqrt(spread + epsilon)


def triangle(pieces):
    return jnp.einsum(
        "gcik,gcjk->gcij", pieces[0], pieces[1], preferred_element_type=jnp.float32
    ).astype(jnp.bfloat16)


def evo_block(current, mask_all, proj_mats, out_mat, up_mat, down_mat, gain_rows):
    row_count = current.shape[0]
    width = current.shape[1]
    channels = current.shape[2]
    group_count = lax.axis_size("axial")
    per_group = channels // group_count
    row_start = lax.axis_index("axial") * row_count
    mask_rows = lax.dynamic_slice_in_dim(mask_all, row_start, row_count)
    gain_vals = gain_rows.astype(jnp.float32)
    pair_f = current.astype(jnp.float32)
    normed = (normalize(pair_f, 2) * gain_vals[0]).astype(jnp.bfloat16)
    linear = jnp.einsum("rnd,edc->ecrn", normed, proj_mats[:4], preferred_element_type=jnp.float32)
    pair_mask = mask_rows[:, None] * mask_all[None, :]
    left_edge = (jax.nn.sigmoid(linear[1]) * linear[0] * pair_mask).astype(jnp.bfloat16)
    right_edge = (jax.nn.sigmoid(linear[3]) * linear[2] * pair_mask).astype(jnp.bfloat16)
    left_groups = left_edge.reshape(group_count, per_group, row_count, width)
    right_groups = right_edge.reshape(group_count, per_group, row_count, width)
    product = triangle(
        (
            lax.all_to_all(left_groups, "axial", split_axis=0, concat_axis=2, tiled=True),
            lax.all_to_all(right_groups, "axial", split_axis=0, concat_axis=2, tiled=True),
        )
    )
    restored = lax.all_to_all(product, "axial", split_axis=2, concat_axis=0, tiled=True).reshape(
        channels, row_count, width
    )
    tri_norm = (normalize(restored.astype(jnp.float32), 0) * gain_vals[1][:, None, None]).astype(
        jnp.bfloat16
    )
    update = jnp.einsum("crn,cd->rnd", tri_norm, out_mat, preferred_element_type=jnp.float32)
    gate_values = jax.nn.sigmoid(
        jnp.einsum("rnd,dc->rnc", normed, proj_mats[4], preferred_element_type=jnp.float32)
    )
    pair_mid = pair_f + gate_values * update
    trans_in = (normalize(pair_mid, 2) * gain_vals[2]).astype(jnp.bfloat16).reshape(-1, channels)
    hidden = jax.nn.relu(jnp.dot(trans_in, up_mat, preferred_element_type=jnp.float32)).astype(
        jnp.bfloat16
    )
    pair_new = pair_mid + jnp.dot(hidden, down_mat, preferred_element_type=jnp.float32).reshape(
        pair_mid.shape
    )
    return pair_new.astype(jnp.bfloat16)


MESH = pl.DeviceIdType.MESH


def sigmoid(values):
    return 0.5 * jnp.tanh(0.5 * values) + 0.5


def normalize_rows(values, gain):
    scale = 1.0 / values.shape[0]
    center = values - jnp.sum(values, axis=0, keepdims=True) * scale
    spread = jnp.sum(center * center, axis=0, keepdims=True) * scale
    return center * lax.rsqrt(spread + epsilon) * gain


def matmul(mat, values):
    return lax.dot_general(mat, values, (((1,), (0,)), ((), ())), preferred_element_type=jnp.float32)


def fused_kernel(
    sections,
    ranks,
    halves,
    own_count,
    sub_rows,
    pair_ref,
    mask_ref,
    mask_smem,
    proj_ref,
    out_ref,
    up_ref,
    down_ref,
    gain_ref,
    result_ref,
    pair_buf,
    z_buf,
    normed_buf,
    gate_buf,
    edge_send,
    edge_recv,
    tri_send,
    tri_recv,
    left_f,
    right_f,
    tri_f,
    result_buf,
    proj_raw,
    out_raw,
    up_raw,
    down_raw,
    gain_all,
    proj_t,
    out_t,
    up_t,
    down_t,
    gain_t,
    pair_send_sem,
    pair_sem,
    edge_send_sem,
    edge_recv_sem,
    tri_send_sem,
    tri_recv_sem,
    result_send_sem,
    result_recv_sem,
    raw_sem,
    weight_send_sem,
    weight_pass_sem,
    weight_sem,
):
    section = lax.axis_index("section")
    axial = lax.axis_index("axial")
    span = ranks // sections
    group = axial // span
    place = lax.rem(axial, span)
    core = lax.rem(axial, 2)
    rank = section * span + place
    piece_rows, width, channels = pair_buf.shape[2:]
    rows = piece_rows * sections
    owners = ranks // halves
    per_group = channels // owners
    my_half = rank // owners
    my_owner = lax.rem(rank, owners)
    steps = piece_rows // sub_rows
    everyone = range(own_count)
    pieces = range(sections)

    def member(index):
        return {"section": index // span, "axial": group * span + lax.rem(index, span)}

    def part_of(t):
        return lax.rem(group + t, sections)

    def first_row(t, section_at, place_at):
        return (part_of(t) * span + place_at) * rows + section_at * piece_rows

    own_rows = pl.ds(section * piece_rows, piece_rows)

    for m in everyone:
        pltpu.make_async_copy(
            pair_ref.at[group * own_count + m, own_rows], pair_buf.at[m, 0], pair_sem.at[m, 0]
        ).start()
    raw_copies = [
        pltpu.make_async_copy(source, target, raw_sem.at[index])
        for index, (source, target) in enumerate(
            (
                (gain_ref.at[0], gain_all.at[section]),
                (proj_ref.at[0, pl.ds(2, 2)], proj_raw.at[pl.ds(2, 2)]),
                (proj_ref.at[0, pl.ds(0, 2)], proj_raw.at[pl.ds(0, 2)]),
                (proj_ref.at[0, pl.ds(4, 1)], proj_raw.at[pl.ds(4, 1)]),
                (out_ref.at[0], out_raw),
                (up_ref.at[0], up_raw),
                (down_ref.at[0], down_raw),
            )
        )
    ]
    for copy in raw_copies:
        copy.start()

    barrier = pltpu.get_barrier_semaphore()
    for k in range(1, ranks):
        pl.semaphore_signal(
            barrier, inc=1, device_id=member(lax.rem(rank + k, ranks)), device_id_type=MESH
        )
    for k in range(1, sections):
        for j in range(sections):
            pl.semaphore_signal(
                barrier,
                inc=1,
                device_id={
                    "section": lax.rem(section + j, sections),
                    "axial": part_of(k) * span + place,
                },
                device_id_type=MESH,
            )

    items = (
        (0, lambda layer: gain_all.at[layer]),
        (0, lambda layer: proj_t.at[layer, 2]),
        (1, lambda layer: proj_t.at[layer, 3]),
        (0, lambda layer: proj_t.at[layer, 0]),
        (1, lambda layer: proj_t.at[layer, 1]),
        (0, lambda layer: proj_t.at[layer, 4]),
        (1, lambda layer: out_t.at[layer]),
        (0, lambda layer: up_t.at[layer]),
        (1, lambda layer: down_t.at[layer]),
    )

    def item_copy(a, k):
        view = items[a][1](section)
        return pltpu.make_async_remote_copy(
            src_ref=view,
            dst_ref=view,
            send_sem=weight_send_sem.at[a, k],
            recv_sem=weight_sem.at[a, section],
            device_id={"section": lax.rem(section + k, sections)},
            device_id_type=MESH,
        )

    def item_pass(a, layer):
        view = items[a][1](layer)
        return pltpu.make_async_remote_copy(
            src_ref=view,
            dst_ref=view,
            send_sem=weight_pass_sem.at[a, layer],
            recv_sem=weight_sem.at[a, layer],
            device_id={"axial": axial + 1 - 2 * core},
            device_id_type=MESH,
        )

    def send_items(chosen):
        for side in range(2):

            @pl.when(core == side)
            def start():
                for a in chosen:
                    if items[a][0] == side:
                        for k in range(1, sections):
                            item_copy(a, k).start()

    def wait_item(a, layer):
        view = items[a][1](layer)
        pltpu.make_async_copy(view, view, weight_sem.at[a, layer]).wait()

    def pass_items(chosen, layer):
        for side in range(2):

            @pl.when(core == side)
            def give_on():
                for a in chosen:
                    if items[a][0] == side:
                        wait_item(a, layer)
                        item_pass(a, layer).start()

    def wait_items(chosen, layer):
        for side in range(2):

            @pl.when(core == side)
            def receive():
                for a in chosen:
                    if items[a][0] != side:
                        wait_item(a, layer)

    def finish_items():
        for side in range(2):

            @pl.when(core == side)
            def finish():
                for a, (owner, _) in enumerate(items):
                    if owner == side:
                        for k in range(1, sections):
                            item_copy(a, k).wait_send()
                        for k in range(1, sections):
                            item_pass(a, lax.rem(section + k, sections)).wait_send()

    def turned(values):
        return values.astype(jnp.float32).T.astype(jnp.bfloat16)

    def prepare_gains(layer):
        for index in range(gain_t.shape[1]):
            row = gain_all[layer, index : index + 1, :].astype(jnp.float32)
            gain_t[layer, index] = jnp.broadcast_to(row, (width, channels)).T

    def prepare_edges():
        raw_copies[0].wait()
        for pair in (1, 0):
            raw_copies[2 - pair].wait()
            for e in (2 * pair, 2 * pair + 1):
                proj_t[section, e] = turned(proj_raw[e])

    def prepare_rest():
        raw_copies[3].wait()
        proj_t[section, 4] = turned(proj_raw[4])
        for copy in raw_copies[4:]:
            copy.wait()
        out_t[section] = turned(out_raw[...])
        up_t[section] = turned(up_raw[...])
        down_t[section] = turned(down_raw[...])

    def wide_gain(layer, index):
        return jnp.concatenate([gain_t[layer, index]] * sub_rows, axis=1)

    def pair_copy(m, k):
        target = part_of(k)
        return pltpu.make_async_remote_copy(
            src_ref=pair_ref.at[target * own_count + m, own_rows],
            dst_ref=pair_buf.at[m, sections - k],
            send_sem=pair_send_sem.at[m, k],
            recv_sem=pair_sem.at[m, sections - k],
            device_id={"axial": target * span + place},
            device_id_type=MESH,
        )

    def load_pair(m, t):
        pltpu.make_async_copy(pair_buf.at[m, t], pair_buf.at[m, t], pair_sem.at[m, t]).wait()
        for q in range(steps):
            for i in range(sub_rows):
                z_buf[m, t, q, :, i * width : (i + 1) * width] = (
                    pair_buf[m, t, q * sub_rows + i].astype(jnp.float32).T
                )

    def phase_norm(layer, m, t):
        for q in range(steps):
            normed_buf[m, t, q] = normalize_rows(z_buf[m, t, q], wide_gain(layer, 0)).astype(
                jnp.bfloat16
            )

    def phase_edges(layer, m, t):
        crop = group * own_count + m
        row_mask = mask_ref[pl.ds(crop, 1), :].astype(jnp.float32)
        start = first_row(t, section, place)
        for q in range(steps):
            values = normed_buf[m, t, q]
            masks = []
            for i in range(sub_rows):
                own = mask_smem[crop, start + q * sub_rows + i]
                masks.append(row_mask * own.astype(jnp.float32))
            pair_mask = jnp.concatenate(masks, axis=1)
            for side in (1, 0):
                value = matmul(proj_t[layer, 2 * side], values)
                gate = matmul(proj_t[layer, 2 * side + 1], values)
                edge = sigmoid(gate) * value * pair_mask
                for i in range(sub_rows):
                    part = edge[:, i * width : (i + 1) * width].reshape(owners, per_group, width)
                    edge_send[m, t, :, side, q * sub_rows + i] = part.astype(jnp.bfloat16)

    def phase_gate(layer, m, t):
        for q in range(steps):
            gate_buf[m, t, q] = sigmoid(matmul(proj_t[layer, 4], normed_buf[m, t, q]))

    def rank_at(half_step, index):
        if halves == 1:
            return index
        return lax.rem(my_half + half_step, halves) * owners + index

    def edge_view(ref, half_step):
        return ref if half_step == 0 else ref.at[1]

    def edge_copy(slot, m, t, k):
        half_step = k // owners
        owner = lax.rem(my_owner + k % owners, owners)
        return pltpu.make_async_remote_copy(
            src_ref=edge_view(edge_send.at[m, t, owner], half_step),
            dst_ref=edge_view(edge_recv.at[slot, m, t, rank], half_step),
            send_sem=edge_send_sem.at[m, t],
            recv_sem=edge_recv_sem.at[slot, m, t],
            device_id=member(rank_at(half_step, owner)),
            device_id_type=MESH,
        )

    def send_edges(slot, m, t):
        for k in range(ranks - 1, 0, -1):
            edge_copy(slot, m, t, k).start()
        pltpu.make_async_copy(
            edge_send.at[m, t, my_owner],
            edge_recv.at[slot, m, t, rank],
            edge_recv_sem.at[slot, m, t],
        ).start()

    def wait_edges_sent(m, t):
        left_over = (halves - 1) * owners
        sent = edge_recv.at[0, m, t, pl.ds(0, owners - 1 + left_over // 2)]
        pltpu.make_async_copy(sent, sent, edge_send_sem.at[m, t]).wait()

    def wait_edges(slot, m, t):
        left_over = (halves - 1) * owners
        got = edge_recv.at[slot, m, t, pl.ds(0, owners + left_over // 2)]
        pltpu.make_async_copy(got, got, edge_recv_sem.at[slot, m, t]).wait()

    def tri_copy(m, k):
        owner = lax.rem(my_owner + k, owners)
        return pltpu.make_async_remote_copy(
            src_ref=tri_send.at[m, owner],
            dst_ref=tri_recv.at[m, my_owner],
            send_sem=tri_send_sem.at[m],
            recv_sem=tri_recv_sem.at[m],
            device_id=member(my_half * owners + owner),
            device_id_type=MESH,
        )

    def send_tri(m):
        for k in range(owners - 1, 0, -1):
            tri_copy(m, k).start()
        pltpu.make_async_copy(
            tri_send.at[m, my_owner], tri_recv.at[m, my_owner], tri_recv_sem.at[m]
        ).start()

    def wait_tri_sent(m):
        sent = tri_recv.at[m, pl.ds(0, owners - 1)]
        pltpu.make_async_copy(sent, sent, tri_send_sem.at[m]).wait()

    def wait_tri(m):
        pltpu.make_async_copy(tri_recv.at[m], tri_recv.at[m], tri_recv_sem.at[m]).wait()

    def phase_triangle(slot, m):
        for t in pieces:
            wait_edges(slot, m, t)
            for half_step in range(halves):
                for index in range(owners):
                    g = rank_at(half_step, index)
                    start = first_row(t, g // span, g % span if halves == 1 else lax.rem(g, span))
                    right_f[pl.ds(start, piece_rows)] = edge_recv[slot, m, t, g, 1].astype(
                        jnp.float32
                    )
                    if half_step == 0:
                        at = index * rows + t * piece_rows
                        left_f[at : at + piece_rows] = edge_recv[slot, m, t, g, 0].astype(
                            jnp.float32
                        )
        for c in range(per_group):
            tri_f[:, c, :] = lax.dot_general(
                left_f[:, c, :].astype(jnp.bfloat16),
                right_f[:, c, :].astype(jnp.bfloat16),
                (((1,), (1,)), ((), ())),
                preferred_element_type=jnp.float32,
            )
        for g in range(owners):
            tri_send[m, g] = tri_f[g * rows : (g + 1) * rows].astype(jnp.bfloat16)

    def phase_update(layer, m, t, last):
        for q in range(steps):
            parts = []
            for i in range(sub_rows):
                part = tri_recv[m, :, t * piece_rows + q * sub_rows + i].astype(jnp.float32)
                parts.append(part.reshape(channels, width))
            tri = jnp.concatenate(parts, axis=1)
            tri_norm = normalize_rows(tri, wide_gain(layer, 1)).astype(jnp.bfloat16)
            mid = z_buf[m, t, q] + gate_buf[m, t, q] * matmul(out_t[layer], tri_norm)
            trans_in = normalize_rows(mid, wide_gain(layer, 2)).astype(jnp.bfloat16)
            hidden = jnp.maximum(matmul(up_t[layer], trans_in), 0.0).astype(jnp.bfloat16)
            fresh = mid + matmul(down_t[layer], hidden)
            if last:
                for i in range(sub_rows):
                    part = fresh[:, i * width : (i + 1) * width]
                    result_buf[m, t, q * sub_rows + i] = part.T.astype(jnp.bfloat16)
            else:
                z_buf[m, t, q] = fresh.astype(jnp.bfloat16).astype(jnp.float32)

    def result_copy(m, t):
        return pltpu.make_async_remote_copy(
            src_ref=result_buf.at[m, t],
            dst_ref=result_ref.at[m, own_rows],
            send_sem=result_send_sem.at[m, t],
            recv_sem=result_recv_sem.at[m, section],
            device_id={"section": group, "axial": part_of(t) * span + place},
            device_id_type=MESH,
        )

    def send_result(m, t):
        if t > 0:
            result_copy(m, t).start()
            return

        @pl.when(section == group)
        def keep():
            pltpu.make_async_copy(
                result_buf.at[m, t], result_ref.at[m, own_rows], result_recv_sem.at[m, section]
            ).start()

        @pl.when(section != group)
        def give():
            result_copy(m, t).start()

    def finish_results():
        for m in everyone:
            for t in pieces:
                if t > 0:
                    result_copy(m, t).wait_send()
                else:

                    @pl.when(section != group)
                    def given():
                        result_copy(m, t).wait_send()

            for s in range(sections):
                part = result_ref.at[m, pl.ds(s * piece_rows, piece_rows)]
                pltpu.make_async_copy(part, part, result_recv_sem.at[m, s]).wait()

    edge_items = range(5)
    rest_items = range(5, len(items))
    prepare_edges()
    pl.semaphore_wait(barrier, ranks - 1 + (sections - 1) * sections)

    @pl.when(section == 0)
    def first_items():
        send_items(edge_items)

    for k in range(1, sections):
        pair_copy(0, k).start()
    prepare_gains(section)

    @pl.when(section != 0)
    def other_items():
        prepare_rest()
        send_items(range(len(items)))

    for m in everyone:
        load_pair(m, 0)

    @pl.when(section != 0)
    def first_weights():
        pass_items(edge_items, 0)
        wait_items(edge_items, 0)
        prepare_gains(0)

    phase_norm(0, 0, 0)
    phase_edges(0, 0, 0)
    send_edges(0, 0, 0)
    for m in everyone[1:]:
        for k in range(1, sections):
            pair_copy(m, k).start()

    @pl.when(section == 0)
    def second_items():
        prepare_rest()
        send_items(rest_items)

    for m in everyone[1:]:
        phase_norm(0, m, 0)
        phase_edges(0, m, 0)
    for other in range(1, sections):

        @pl.when(section != other)
        def relay_later():
            pass_items(range(len(items)), other)

    for m in everyone:
        for t in pieces[1:]:
            load_pair(m, t)
            phase_norm(0, m, t)
            phase_edges(0, m, t)
            send_edges(0, m, t)
        if m == 0:

            @pl.when(section != 0)
            def relay_first():
                pass_items(rest_items, 0)

        if m + 1 < own_count:
            send_edges(0, m + 1, 0)

    @pl.when(section != 0)
    def other_weights():
        wait_items(rest_items, 0)

    for m in everyone:
        for t in pieces:
            phase_gate(0, m, t)

    for layer in range(sections):
        last = layer == sections - 1
        for m in everyone:
            if layer > 0:
                wait_tri_sent(m)
            phase_triangle(layer % 2, m)
            send_tri(m)
        if layer == 0:
            for other in range(1, sections):

                @pl.when(section != other)
                def later_weights():
                    wait_items(range(len(items)), other)
                    prepare_gains(other)

        for m in everyone:
            wait_tri(m)
            for t in pieces:
                phase_update(layer, m, t, last)
                wait_edges_sent(m, t)
                if last:
                    send_result(m, t)
                else:
                    phase_norm(layer + 1, m, t)
                    phase_edges(layer + 1, m, t)
                    send_edges((layer + 1) % 2, m, t)
        if not last:
            for m in everyone:
                for t in pieces:
                    phase_gate(layer + 1, m, t)
    for m in everyone:
        wait_tri_sent(m)
        for k in range(1, sections):
            pair_copy(m, k).wait_send()
    finish_items()
    finish_results()


def fused_device(pair_in, crop_mask, proj_weights, out_weights, up_weights, down_weights, norm_gains):
    sections = lax.axis_size("section")
    ranks = lax.axis_size("axial")
    micro_count, rows, width, channels = pair_in.shape
    own_count = micro_count // sections
    halves = half_count(pair_in)
    owners = ranks // halves
    per_group = channels // owners
    piece_rows = rows // sections
    sub_rows = 2 if piece_rows % 2 == 0 else 1
    steps = piece_rows // sub_rows
    lanes = sub_rows * width
    hidden = up_weights.shape[2]
    gains = norm_gains.shape[1]
    edge_kinds = proj_weights.shape[1]
    bf16, f32 = jnp.bfloat16, jnp.float32
    vmem = pl.BlockSpec(memory_space=pltpu.VMEM)
    hbm = pl.BlockSpec(memory_space=pltpu.HBM)
    dma = pltpu.SemaphoreType.DMA
    piece = (piece_rows, per_group, width)
    rows_shape = (own_count, sections, piece_rows, width, channels)
    wide_shape = (own_count, sections, steps, channels, lanes)
    tri_shape = (own_count, owners, rows, per_group, width)
    return pl.pallas_call(
        functools.partial(fused_kernel, sections, ranks, halves, own_count, sub_rows),
        out_shape=jax.ShapeDtypeStruct((own_count, rows, width, channels), bf16),
        in_specs=[hbm, vmem, pl.BlockSpec(memory_space=pltpu.SMEM)] + [hbm] * 5,
        out_specs=hbm,
        scratch_shapes=[
            pltpu.VMEM(rows_shape, bf16),
            pltpu.VMEM(wide_shape, f32),
            pltpu.VMEM(wide_shape, bf16),
            pltpu.VMEM(wide_shape, f32),
            pltpu.VMEM((own_count, sections, owners, 2) + piece, bf16),
            pltpu.VMEM((2, own_count, sections, ranks, 2) + piece, bf16),
            pltpu.VMEM(tri_shape, bf16),
            pltpu.VMEM(tri_shape, bf16),
            pltpu.VMEM((owners * rows, per_group, width), f32),
            pltpu.VMEM((ranks * rows, per_group, width), f32),
            pltpu.VMEM((owners * rows, per_group, width), f32),
            pltpu.VMEM(rows_shape, bf16),
            pltpu.VMEM(proj_weights.shape[1:], bf16),
            pltpu.VMEM(out_weights.shape[1:], bf16),
            pltpu.VMEM(up_weights.shape[1:], bf16),
            pltpu.VMEM(down_weights.shape[1:], bf16),
            pltpu.VMEM((sections,) + norm_gains.shape[1:], bf16),
            pltpu.VMEM((sections, edge_kinds, channels, channels), bf16),
            pltpu.VMEM((sections, channels, channels), bf16),
            pltpu.VMEM((sections, hidden, channels), bf16),
            pltpu.VMEM((sections, channels, hidden), bf16),
            pltpu.VMEM((sections, gains, channels, width), f32),
            dma((own_count, sections)),
            dma((own_count, sections)),
            dma((own_count, sections)),
            dma((2, own_count, sections)),
            dma((own_count,)),
            dma((own_count,)),
            dma((own_count, sections)),
            dma((own_count, sections)),
            dma((7,)),
            dma((9, sections)),
            dma((9, sections)),
            dma((9, sections)),
        ],
        compiler_params=pltpu.CompilerParams(
            collective_id=0, has_side_effects=True, vmem_limit_bytes=67043328
        ),
    )(
        pair_in,
        crop_mask,
        crop_mask,
        proj_weights,
        out_weights,
        up_weights,
        down_weights,
        norm_gains,
    )


def half_count(pair_in):
    ranks = lax.axis_size("axial")
    return 2 if ranks % 2 == 0 and pair_in.shape[3] % (8 * ranks) else 1


def fits_fused(pair_in):
    rows, width, channels = pair_in.shape[1:]
    sections = lax.axis_size("section")
    ranks = lax.axis_size("axial")
    owners = ranks // half_count(pair_in)
    return (
        channels % (8 * owners) == 0
        and rows % sections == 0
        and width % 128 == 0
        and ranks % (2 * sections) == 0
    )


def per_device(pair_in, crop_mask, proj_weights, out_weights, up_weights, down_weights, norm_gains):
    if fits_fused(pair_in):
        return fused_device(
            pair_in, crop_mask, proj_weights, out_weights, up_weights, down_weights, norm_gains
        )
    section_index = lax.axis_index("section")
    section_count = lax.axis_size("section")
    micro_count = pair_in.shape[0]
    own_count = micro_count // section_count
    gathered = (
        lax.all_gather(proj_weights, "section", axis=0, tiled=True),
        lax.all_gather(out_weights, "section", axis=0, tiled=True),
        lax.all_gather(up_weights, "section", axis=0, tiled=True),
        lax.all_gather(down_weights, "section", axis=0, tiled=True),
        lax.all_gather(norm_gains, "section", axis=0, tiled=True),
    )
    own_pairs = lax.dynamic_slice_in_dim(pair_in, section_index * own_count, own_count, 0)
    own_masks = lax.dynamic_slice_in_dim(crop_mask, section_index * own_count, own_count, 0).astype(
        jnp.float32
    )
    outputs = []
    for member in range(own_count):
        current = own_pairs[member]
        for layer_index in range(section_count):
            current = evo_block(
                current,
                own_masks[member],
                gathered[0][layer_index],
                gathered[1][layer_index],
                gathered[2][layer_index],
                gathered[3][layer_index],
                gathered[4][layer_index],
            )
        outputs.append(current)
    return jnp.stack(outputs)


def solution(mesh):
    return jax.shard_map(
        per_device,
        mesh=mesh,
        in_specs=(
            P("groups", "axial", None, None),
            P("groups", None),
            P("section", None, None, None),
            P("section", None, None),
            P("section", None, None),
            P("section", None, None),
            P("section", None, None),
        ),
        out_specs=P(("groups", "section"), "axial", None, None),
        check_vma=False,
    )
```

```python
import functools

import jax
import jax.numpy as jnp
from jax import lax
from jax.experimental import pallas as pl
from jax.experimental.pallas import tpu as pltpu
from jax.sharding import PartitionSpec as P

epsilon = 1e-05


def normalize(values, axis_dim):
    center = values - jnp.mean(values, axis=axis_dim, keepdims=True)
    spread = jnp.mean(center * center, axis=axis_dim, keepdims=True)
    return center * lax.rsqrt(spread + epsilon)


def triangle(pieces):
    return jnp.einsum(
        "gcik,gcjk->gcij", pieces[0], pieces[1], preferred_element_type=jnp.float32
    ).astype(jnp.bfloat16)


def evo_block(current, mask_all, proj_mats, out_mat, up_mat, down_mat, gain_rows):
    row_count = current.shape[0]
    width = current.shape[1]
    channels = current.shape[2]
    group_count = lax.axis_size("axial")
    per_group = channels // group_count
    row_start = lax.axis_index("axial") * row_count
    mask_rows = lax.dynamic_slice_in_dim(mask_all, row_start, row_count)
    gain_vals = gain_rows.astype(jnp.float32)
    pair_f = current.astype(jnp.float32)
    normed = (normalize(pair_f, 2) * gain_vals[0]).astype(jnp.bfloat16)
    linear = jnp.einsum("rnd,edc->ecrn", normed, proj_mats[:4], preferred_element_type=jnp.float32)
    pair_mask = mask_rows[:, None] * mask_all[None, :]
    left_edge = (jax.nn.sigmoid(linear[1]) * linear[0] * pair_mask).astype(jnp.bfloat16)
    right_edge = (jax.nn.sigmoid(linear[3]) * linear[2] * pair_mask).astype(jnp.bfloat16)
    left_groups = left_edge.reshape(group_count, per_group, row_count, width)
    right_groups = right_edge.reshape(group_count, per_group, row_count, width)
    product = triangle(
        (
            lax.all_to_all(left_groups, "axial", split_axis=0, concat_axis=2, tiled=True),
            lax.all_to_all(right_groups, "axial", split_axis=0, concat_axis=2, tiled=True),
        )
    )
    restored = lax.all_to_all(product, "axial", split_axis=2, concat_axis=0, tiled=True).reshape(
        channels, row_count, width
    )
    tri_norm = (normalize(restored.astype(jnp.float32), 0) * gain_vals[1][:, None, None]).astype(
        jnp.bfloat16
    )
    update = jnp.einsum("crn,cd->rnd", tri_norm, out_mat, preferred_element_type=jnp.float32)
    gate_values = jax.nn.sigmoid(
        jnp.einsum("rnd,dc->rnc", normed, proj_mats[4], preferred_element_type=jnp.float32)
    )
    pair_mid = pair_f + gate_values * update
    trans_in = (normalize(pair_mid, 2) * gain_vals[2]).astype(jnp.bfloat16).reshape(-1, channels)
    hidden = jax.nn.relu(jnp.dot(trans_in, up_mat, preferred_element_type=jnp.float32)).astype(
        jnp.bfloat16
    )
    pair_new = pair_mid + jnp.dot(hidden, down_mat, preferred_element_type=jnp.float32).reshape(
        pair_mid.shape
    )
    return pair_new.astype(jnp.bfloat16)


MESH = pl.DeviceIdType.MESH


def sigmoid(values):
    return 0.5 * jnp.tanh(0.5 * values) + 0.5


def normalize_rows(values, gain):
    scale = 1.0 / values.shape[0]
    center = values - jnp.sum(values, axis=0, keepdims=True) * scale
    spread = jnp.sum(center * center, axis=0, keepdims=True) * scale
    return center * lax.rsqrt(spread + epsilon) * gain


def matmul(mat, values):
    return lax.dot_general(mat, values, (((1,), (0,)), ((), ())), preferred_element_type=jnp.float32)


def fused_kernel(
    sections,
    ranks,
    halves,
    own_count,
    sub_rows,
    pair_ref,
    mask_ref,
    mask_smem,
    proj_ref,
    out_ref,
    up_ref,
    down_ref,
    gain_ref,
    result_ref,
    pair_buf,
    z_buf,
    normed_buf,
    gate_buf,
    edge_send,
    edge_recv,
    tri_send,
    tri_recv,
    left_f,
    right_f,
    tri_f,
    result_buf,
    proj_raw,
    out_raw,
    up_raw,
    down_raw,
    gain_all,
    proj_t,
    out_t,
    up_t,
    down_t,
    gain_t,
    pair_send_sem,
    pair_sem,
    edge_send_sem,
    edge_recv_sem,
    tri_send_sem,
    tri_recv_sem,
    result_send_sem,
    result_recv_sem,
    raw_sem,
    weight_send_sem,
    weight_pass_sem,
    weight_sem,
):
    section = lax.axis_index("section")
    axial = lax.axis_index("axial")
    span = ranks // sections
    group = axial // span
    place = lax.rem(axial, span)
    core = lax.rem(axial, 2)
    rank = section * span + place
    piece_rows, width, channels = pair_buf.shape[2:]
    rows = piece_rows * sections
    owners = ranks // halves
    per_group = channels // owners
    my_half = rank // owners
    my_owner = lax.rem(rank, owners)
    steps = piece_rows // sub_rows
    everyone = range(own_count)
    pieces = range(sections)

    def member(index):
        return {"section": index // span, "axial": group * span + lax.rem(index, span)}

    def part_of(t):
        return lax.rem(group + t, sections)

    def first_row(t, section_at, place_at):
        return (part_of(t) * span + place_at) * rows + section_at * piece_rows

    own_rows = pl.ds(section * piece_rows, piece_rows)

    for m in everyone:
        pltpu.make_async_copy(
            pair_ref.at[group * own_count + m, own_rows], pair_buf.at[m, 0], pair_sem.at[m, 0]
        ).start()
    raw_copies = [
        pltpu.make_async_copy(source, target, raw_sem.at[index])
        for index, (source, target) in enumerate(
            (
                (gain_ref.at[0], gain_all.at[section]),
                (proj_ref.at[0, pl.ds(2, 2)], proj_raw.at[pl.ds(2, 2)]),
                (proj_ref.at[0, pl.ds(0, 2)], proj_raw.at[pl.ds(0, 2)]),
                (proj_ref.at[0, pl.ds(4, 1)], proj_raw.at[pl.ds(4, 1)]),
                (out_ref.at[0], out_raw),
                (up_ref.at[0], up_raw),
                (down_ref.at[0], down_raw),
            )
        )
    ]
    for copy in raw_copies:
        copy.start()

    barrier = pltpu.get_barrier_semaphore()
    for k in range(1, ranks):
        pl.semaphore_signal(
            barrier, inc=1, device_id=member(lax.rem(rank + k, ranks)), device_id_type=MESH
        )
    for k in range(1, sections):
        for j in range(sections):
            pl.semaphore_signal(
                barrier,
                inc=1,
                device_id={
                    "section": lax.rem(section + j, sections),
                    "axial": part_of(k) * span + place,
                },
                device_id_type=MESH,
            )

    items = (
        (1, lambda layer: gain_all.at[layer]),
        (1, lambda layer: proj_t.at[layer, 2]),
        (1, lambda layer: proj_t.at[layer, 3]),
        (1, lambda layer: proj_t.at[layer, 0]),
        (1, lambda layer: proj_t.at[layer, 1]),
        (1, lambda layer: proj_t.at[layer, 4]),
        (1, lambda layer: out_t.at[layer]),
        (0, lambda layer: up_t.at[layer]),
        (0, lambda layer: down_t.at[layer]),
    )

    def item_copy(a, k):
        view = items[a][1](section)
        return pltpu.make_async_remote_copy(
            src_ref=view,
            dst_ref=view,
            send_sem=weight_send_sem.at[a, k],
            recv_sem=weight_sem.at[a, section],
            device_id={"section": lax.rem(section + k, sections)},
            device_id_type=MESH,
        )

    def item_pass(a, layer):
        view = items[a][1](layer)
        return pltpu.make_async_remote_copy(
            src_ref=view,
            dst_ref=view,
            send_sem=weight_pass_sem.at[a, layer],
            recv_sem=weight_sem.at[a, layer],
            device_id={"axial": axial + 1 - 2 * core},
            device_id_type=MESH,
        )

    def send_items(chosen):
        for side in range(2):

            @pl.when(core == side)
            def start():
                for a in chosen:
                    if items[a][0] == side:
                        for k in range(1, sections):
                            item_copy(a, k).start()

    def wait_item(a, layer):
        view = items[a][1](layer)
        pltpu.make_async_copy(view, view, weight_sem.at[a, layer]).wait()

    def pass_items(chosen, layer):
        for side in range(2):

            @pl.when(core == side)
            def give_on():
                for a in chosen:
                    if items[a][0] == side:
                        wait_item(a, layer)
                        item_pass(a, layer).start()

    def wait_items(chosen, layer):
        for side in range(2):

            @pl.when(core == side)
            def receive():
                for a in chosen:
                    if items[a][0] != side:
                        wait_item(a, layer)

    def finish_items():
        for side in range(2):

            @pl.when(core == side)
            def finish():
                for a, (owner, _) in enumerate(items):
                    if owner == side:
                        for k in range(1, sections):
                            item_copy(a, k).wait_send()
                        for k in range(1, sections):
                            item_pass(a, lax.rem(section + k, sections)).wait_send()

    def turned(values):
        return values.astype(jnp.float32).T.astype(jnp.bfloat16)

    def prepare_gains(layer):
        for index in range(gain_t.shape[1]):
            row = gain_all[layer, index : index + 1, :].astype(jnp.float32)
            gain_t[layer, index] = jnp.broadcast_to(row, (width, channels)).T

    def prepare_edges():
        raw_copies[0].wait()
        for pair in (1, 0):
            raw_copies[2 - pair].wait()
            for e in (2 * pair, 2 * pair + 1):
                proj_t[section, e] = turned(proj_raw[e])

    def prepare_rest():
        raw_copies[3].wait()
        proj_t[section, 4] = turned(proj_raw[4])
        for copy in raw_copies[4:]:
            copy.wait()
        out_t[section] = turned(out_raw[...])
        up_t[section] = turned(up_raw[...])
        down_t[section] = turned(down_raw[...])

    def wide_gain(layer, index):
        return jnp.concatenate([gain_t[layer, index]] * sub_rows, axis=1)

    def pair_copy(m, k):
        target = part_of(k)
        return pltpu.make_async_remote_copy(
            src_ref=pair_ref.at[target * own_count + m, own_rows],
            dst_ref=pair_buf.at[m, sections - k],
            send_sem=pair_send_sem.at[m, k],
            recv_sem=pair_sem.at[m, sections - k],
            device_id={"axial": target * span + place},
            device_id_type=MESH,
        )

    def load_pair(m, t):
        pltpu.make_async_copy(pair_buf.at[m, t], pair_buf.at[m, t], pair_sem.at[m, t]).wait()
        for q in range(steps):
            for i in range(sub_rows):
                z_buf[m, t, q, :, i * width : (i + 1) * width] = (
                    pair_buf[m, t, q * sub_rows + i].astype(jnp.float32).T
                )

    def phase_norm(layer, m, t):
        for q in range(steps):
            normed_buf[m, t, q] = normalize_rows(z_buf[m, t, q], wide_gain(layer, 0)).astype(
                jnp.bfloat16
            )

    def phase_edges(layer, m, t):
        crop = group * own_count + m
        row_mask = mask_ref[pl.ds(crop, 1), :].astype(jnp.float32)
        start = first_row(t, section, place)
        for q in range(steps):
            values = normed_buf[m, t, q]
            masks = []
            for i in range(sub_rows):
                own = mask_smem[crop, start + q * sub_rows + i]
                masks.append(row_mask * own.astype(jnp.float32))
            pair_mask = jnp.concatenate(masks, axis=1)
            for side in (1, 0):
                value = matmul(proj_t[layer, 2 * side], values)
                gate = matmul(proj_t[layer, 2 * side + 1], values)
                edge = sigmoid(gate) * value * pair_mask
                for i in range(sub_rows):
                    part = edge[:, i * width : (i + 1) * width].reshape(owners, per_group, width)
                    edge_send[m, t, :, side, q * sub_rows + i] = part.astype(jnp.bfloat16)

    def phase_gate(layer, m, t):
        for q in range(steps):
            gate_buf[m, t, q] = sigmoid(matmul(proj_t[layer, 4], normed_buf[m, t, q]))

    def rank_at(half_step, index):
        if halves == 1:
            return index
        return lax.rem(my_half + half_step, halves) * owners + index

    def edge_view(ref, half_step):
        return ref if half_step == 0 else ref.at[1]

    def edge_copy(slot, m, t, k):
        half_step = k // owners
        owner = lax.rem(my_owner + k % owners, owners)
        return pltpu.make_async_remote_copy(
            src_ref=edge_view(edge_send.at[m, t, owner], half_step),
            dst_ref=edge_view(edge_recv.at[slot, m, t, rank], half_step),
            send_sem=edge_send_sem.at[m, t],
            recv_sem=edge_recv_sem.at[slot, m, t],
            device_id=member(rank_at(half_step, owner)),
            device_id_type=MESH,
        )

    def send_edges(slot, m, t):
        for k in range(ranks - 1, 0, -1):
            edge_copy(slot, m, t, k).start()
        pltpu.make_async_copy(
            edge_send.at[m, t, my_owner],
            edge_recv.at[slot, m, t, rank],
            edge_recv_sem.at[slot, m, t],
        ).start()

    def wait_edges_sent(m, t):
        left_over = (halves - 1) * owners
        sent = edge_recv.at[0, m, t, pl.ds(0, owners - 1 + left_over // 2)]
        pltpu.make_async_copy(sent, sent, edge_send_sem.at[m, t]).wait()

    def wait_edges(slot, m, t):
        left_over = (halves - 1) * owners
        got = edge_recv.at[slot, m, t, pl.ds(0, owners + left_over // 2)]
        pltpu.make_async_copy(got, got, edge_recv_sem.at[slot, m, t]).wait()

    def tri_copy(m, k):
        owner = lax.rem(my_owner + k, owners)
        return pltpu.make_async_remote_copy(
            src_ref=tri_send.at[m, owner],
            dst_ref=tri_recv.at[m, my_owner],
            send_sem=tri_send_sem.at[m],
            recv_sem=tri_recv_sem.at[m],
            device_id=member(my_half * owners + owner),
            device_id_type=MESH,
        )

    def send_tri(m):
        for k in range(owners - 1, 0, -1):
            tri_copy(m, k).start()
        pltpu.make_async_copy(
            tri_send.at[m, my_owner], tri_recv.at[m, my_owner], tri_recv_sem.at[m]
        ).start()

    def wait_tri_sent(m):
        sent = tri_recv.at[m, pl.ds(0, owners - 1)]
        pltpu.make_async_copy(sent, sent, tri_send_sem.at[m]).wait()

    def wait_tri(m):
        pltpu.make_async_copy(tri_recv.at[m], tri_recv.at[m], tri_recv_sem.at[m]).wait()

    def phase_triangle(slot, m):
        for t in pieces:
            wait_edges(slot, m, t)
            for half_step in range(halves):
                for index in range(owners):
                    g = rank_at(half_step, index)
                    start = first_row(t, g // span, g % span if halves == 1 else lax.rem(g, span))
                    right_f[pl.ds(start, piece_rows)] = edge_recv[slot, m, t, g, 1].astype(
                        jnp.float32
                    )
                    if half_step == 0:
                        at = index * rows + t * piece_rows
                        left_f[at : at + piece_rows] = edge_recv[slot, m, t, g, 0].astype(
                            jnp.float32
                        )
        for c in range(per_group):
            tri_f[:, c, :] = lax.dot_general(
                left_f[:, c, :].astype(jnp.bfloat16),
                right_f[:, c, :].astype(jnp.bfloat16),
                (((1,), (1,)), ((), ())),
                preferred_element_type=jnp.float32,
            )
        for g in range(owners):
            tri_send[m, g] = tri_f[g * rows : (g + 1) * rows].astype(jnp.bfloat16)

    def phase_update(layer, m, t, last):
        span_q = range(steps)

        def tri_at(q):
            parts = []
            for i in range(sub_rows):
                part = tri_recv[m, :, t * piece_rows + q * sub_rows + i].astype(jnp.float32)
                parts.append(part.reshape(channels, width))
            return jnp.concatenate(parts, axis=1)

        gain_tri, gain_in = wide_gain(layer, 1), wide_gain(layer, 2)
        tri_norm = [normalize_rows(tri_at(q), gain_tri).astype(jnp.bfloat16) for q in span_q]
        update = [matmul(out_t[layer], tri_norm[q]) for q in span_q]
        mid = [z_buf[m, t, q] + gate_buf[m, t, q] * update[q] for q in span_q]
        trans_in = [normalize_rows(mid[q], gain_in).astype(jnp.bfloat16) for q in span_q]
        hidden = [
            jnp.maximum(matmul(up_t[layer], trans_in[q]), 0.0).astype(jnp.bfloat16) for q in span_q
        ]
        fresh = [mid[q] + matmul(down_t[layer], hidden[q]) for q in span_q]
        for q in span_q:
            if last:
                for i in range(sub_rows):
                    part = fresh[q][:, i * width : (i + 1) * width]
                    result_buf[m, t, q * sub_rows + i] = part.T.astype(jnp.bfloat16)
            else:
                z_buf[m, t, q] = fresh[q].astype(jnp.bfloat16).astype(jnp.float32)

    def result_copy(m, t):
        return pltpu.make_async_remote_copy(
            src_ref=result_buf.at[m, t],
            dst_ref=result_ref.at[m, own_rows],
            send_sem=result_send_sem.at[m, t],
            recv_sem=result_recv_sem.at[m, section],
            device_id={"section": group, "axial": part_of(t) * span + place},
            device_id_type=MESH,
        )

    def send_result(m, t):
        if t > 0:
            result_copy(m, t).start()
            return

        @pl.when(section == group)
        def keep():
            pltpu.make_async_copy(
                result_buf.at[m, t], result_ref.at[m, own_rows], result_recv_sem.at[m, section]
            ).start()

        @pl.when(section != group)
        def give():
            result_copy(m, t).start()

    def finish_results():
        for m in everyone:
            for t in pieces:
                if t > 0:
                    result_copy(m, t).wait_send()
                else:

                    @pl.when(section != group)
                    def given():
                        result_copy(m, t).wait_send()

            for s in range(sections):
                part = result_ref.at[m, pl.ds(s * piece_rows, piece_rows)]
                pltpu.make_async_copy(part, part, result_recv_sem.at[m, s]).wait()

    edge_items = range(5)
    rest_items = range(5, len(items))
    prepare_edges()
    pl.semaphore_wait(barrier, ranks - 1 + (sections - 1) * sections)

    @pl.when(section == 0)
    def first_items():
        send_items(edge_items)

    for k in range(1, sections):
        pair_copy(0, k).start()
    prepare_gains(section)

    @pl.when(section != 0)
    def other_items():
        prepare_rest()
        send_items(range(len(items)))

    for m in everyone:
        load_pair(m, 0)

    @pl.when(section != 0)
    def first_weights():
        pass_items(edge_items, 0)
        wait_items(edge_items, 0)
        prepare_gains(0)

    phase_norm(0, 0, 0)
    phase_edges(0, 0, 0)
    send_edges(0, 0, 0)
    for m in everyone[1:]:
        for k in range(1, sections):
            pair_copy(m, k).start()

    @pl.when(section == 0)
    def second_items():
        prepare_rest()
        send_items(rest_items)

    for m in everyone[1:]:
        phase_norm(0, m, 0)
        phase_edges(0, m, 0)
    for other in range(1, sections):

        @pl.when(section != other)
        def relay_later():
            pass_items(range(len(items)), other)

    for m in everyone:
        for t in pieces[1:]:
            load_pair(m, t)
            phase_norm(0, m, t)
            phase_edges(0, m, t)
            send_edges(0, m, t)
        if m == 0:

            @pl.when(section != 0)
            def relay_first():
                pass_items(rest_items, 0)

        if m + 1 < own_count:
            send_edges(0, m + 1, 0)

    @pl.when(section != 0)
    def other_weights():
        wait_items(rest_items, 0)

    for m in everyone:
        for t in pieces:
            phase_gate(0, m, t)

    for layer in range(sections):
        last = layer == sections - 1
        for m in everyone:
            if layer > 0:
                wait_tri_sent(m)
            phase_triangle(layer % 2, m)
            send_tri(m)
        if layer == 0:
            for other in range(1, sections):

                @pl.when(section != other)
                def later_weights():
                    wait_items(range(len(items)), other)
                    prepare_gains(other)

        for m in everyone:
            wait_tri(m)
            for t in pieces:
                phase_update(layer, m, t, last)
                wait_edges_sent(m, t)
                if last:
                    send_result(m, t)
                else:
                    phase_norm(layer + 1, m, t)
                    phase_edges(layer + 1, m, t)
                    send_edges((layer + 1) % 2, m, t)
        if not last:
            for m in everyone:
                for t in pieces:
                    phase_gate(layer + 1, m, t)
    for m in everyone:
        wait_tri_sent(m)
        for k in range(1, sections):
            pair_copy(m, k).wait_send()
    finish_items()
    finish_results()


def fused_device(pair_in, crop_mask, proj_weights, out_weights, up_weights, down_weights, norm_gains):
    sections = lax.axis_size("section")
    ranks = lax.axis_size("axial")
    micro_count, rows, width, channels = pair_in.shape
    own_count = micro_count // sections
    halves = half_count(pair_in)
    owners = ranks // halves
    per_group = channels // owners
    piece_rows = rows // sections
    sub_rows = 2 if piece_rows % 2 == 0 else 1
    steps = piece_rows // sub_rows
    lanes = sub_rows * width
    hidden = up_weights.shape[2]
    gains = norm_gains.shape[1]
    edge_kinds = proj_weights.shape[1]
    bf16, f32 = jnp.bfloat16, jnp.float32
    vmem = pl.BlockSpec(memory_space=pltpu.VMEM)
    hbm = pl.BlockSpec(memory_space=pltpu.HBM)
    dma = pltpu.SemaphoreType.DMA
    piece = (piece_rows, per_group, width)
    rows_shape = (own_count, sections, piece_rows, width, channels)
    wide_shape = (own_count, sections, steps, channels, lanes)
    tri_shape = (own_count, owners, rows, per_group, width)
    return pl.pallas_call(
        functools.partial(fused_kernel, sections, ranks, halves, own_count, sub_rows),
        out_shape=pltpu.VMEM((own_count, rows, width, channels), bf16),
        in_specs=[hbm, vmem, pl.BlockSpec(memory_space=pltpu.SMEM)] + [hbm] * 5,
        out_specs=vmem,
        scratch_shapes=[
            pltpu.VMEM(rows_shape, bf16),
            pltpu.VMEM(wide_shape, f32),
            pltpu.VMEM(wide_shape, bf16),
            pltpu.VMEM(wide_shape, f32),
            pltpu.VMEM((own_count, sections, owners, 2) + piece, bf16),
            pltpu.VMEM((2, own_count, sections, ranks, 2) + piece, bf16),
            pltpu.VMEM(tri_shape, bf16),
            pltpu.VMEM(tri_shape, bf16),
            pltpu.VMEM((owners * rows, per_group, width), f32),
            pltpu.VMEM((ranks * rows, per_group, width), f32),
            pltpu.VMEM((owners * rows, per_group, width), f32),
            pltpu.VMEM(rows_shape, bf16),
            pltpu.VMEM(proj_weights.shape[1:], bf16),
            pltpu.VMEM(out_weights.shape[1:], bf16),
            pltpu.VMEM(up_weights.shape[1:], bf16),
            pltpu.VMEM(down_weights.shape[1:], bf16),
            pltpu.VMEM((sections,) + norm_gains.shape[1:], bf16),
            pltpu.VMEM((sections, edge_kinds, channels, channels), bf16),
            pltpu.VMEM((sections, channels, channels), bf16),
            pltpu.VMEM((sections, hidden, channels), bf16),
            pltpu.VMEM((sections, channels, hidden), bf16),
            pltpu.VMEM((sections, gains, channels, width), f32),
            dma((own_count, sections)),
            dma((own_count, sections)),
            dma((own_count, sections)),
            dma((2, own_count, sections)),
            dma((own_count,)),
            dma((own_count,)),
            dma((own_count, sections)),
            dma((own_count, sections)),
            dma((7,)),
            dma((9, sections)),
            dma((9, sections)),
            dma((9, sections)),
        ],
        compiler_params=pltpu.CompilerParams(
            collective_id=0, has_side_effects=True, vmem_limit_bytes=67043328 - 2 * own_count * rows * width * channels
        ),
    )(
        pair_in,
        crop_mask,
        crop_mask,
        proj_weights,
        out_weights,
        up_weights,
        down_weights,
        norm_gains,
    )


def half_count(pair_in):
    ranks = lax.axis_size("axial")
    return 2 if ranks % 2 == 0 and pair_in.shape[3] % (8 * ranks) else 1


def fits_fused(pair_in):
    rows, width, channels = pair_in.shape[1:]
    sections = lax.axis_size("section")
    ranks = lax.axis_size("axial")
    owners = ranks // half_count(pair_in)
    return (
        channels % (8 * owners) == 0
        and rows % sections == 0
        and width % 128 == 0
        and ranks % (2 * sections) == 0
    )


def per_device(pair_in, crop_mask, proj_weights, out_weights, up_weights, down_weights, norm_gains):
    if fits_fused(pair_in):
        return fused_device(
            pair_in, crop_mask, proj_weights, out_weights, up_weights, down_weights, norm_gains
        )
    section_index = lax.axis_index("section")
    section_count = lax.axis_size("section")
    micro_count = pair_in.shape[0]
    own_count = micro_count // section_count
    gathered = (
        lax.all_gather(proj_weights, "section", axis=0, tiled=True),
        lax.all_gather(out_weights, "section", axis=0, tiled=True),
        lax.all_gather(up_weights, "section", axis=0, tiled=True),
        lax.all_gather(down_weights, "section", axis=0, tiled=True),
        lax.all_gather(norm_gains, "section", axis=0, tiled=True),
    )
    own_pairs = lax.dynamic_slice_in_dim(pair_in, section_index * own_count, own_count, 0)
    own_masks = lax.dynamic_slice_in_dim(crop_mask, section_index * own_count, own_count, 0).astype(
        jnp.float32
    )
    outputs = []
    for member in range(own_count):
        current = own_pairs[member]
        for layer_index in range(section_count):
            current = evo_block(
                current,
                own_masks[member],
                gathered[0][layer_index],
                gathered[1][layer_index],
                gathered[2][layer_index],
                gathered[3][layer_index],
                gathered[4][layer_index],
            )
        outputs.append(current)
    return jnp.stack(outputs)


def solution(mesh):
    return jax.shard_map(
        per_device,
        mesh=mesh,
        in_specs=(
            P("groups", "axial", None, None),
            P("groups", None),
            P("section", None, None, None),
            P("section", None, None),
            P("section", None, None),
            P("section", None, None),
            P("section", None, None),
        ),
        out_specs=P(("groups", "section"), "axial", None, None),
        check_vma=False,
    )
```

```python
import functools

import jax
import jax.numpy as jnp
from jax import lax
from jax.experimental import pallas as pl
from jax.experimental.pallas import tpu as pltpu
from jax.sharding import PartitionSpec as P

epsilon = 1e-05


def normalize(values, axis_dim):
    center = values - jnp.mean(values, axis=axis_dim, keepdims=True)
    spread = jnp.mean(center * center, axis=axis_dim, keepdims=True)
    return center * lax.rsqrt(spread + epsilon)


def triangle(pieces):
    return jnp.einsum(
        "gcik,gcjk->gcij", pieces[0], pieces[1], preferred_element_type=jnp.float32
    ).astype(jnp.bfloat16)


def evo_block(current, mask_all, proj_mats, out_mat, up_mat, down_mat, gain_rows):
    row_count = current.shape[0]
    width = current.shape[1]
    channels = current.shape[2]
    group_count = lax.axis_size("axial")
    per_group = channels // group_count
    row_start = lax.axis_index("axial") * row_count
    mask_rows = lax.dynamic_slice_in_dim(mask_all, row_start, row_count)
    gain_vals = gain_rows.astype(jnp.float32)
    pair_f = current.astype(jnp.float32)
    normed = (normalize(pair_f, 2) * gain_vals[0]).astype(jnp.bfloat16)
    linear = jnp.einsum("rnd,edc->ecrn", normed, proj_mats[:4], preferred_element_type=jnp.float32)
    pair_mask = mask_rows[:, None] * mask_all[None, :]
    left_edge = (jax.nn.sigmoid(linear[1]) * linear[0] * pair_mask).astype(jnp.bfloat16)
    right_edge = (jax.nn.sigmoid(linear[3]) * linear[2] * pair_mask).astype(jnp.bfloat16)
    left_groups = left_edge.reshape(group_count, per_group, row_count, width)
    right_groups = right_edge.reshape(group_count, per_group, row_count, width)
    product = triangle(
        (
            lax.all_to_all(left_groups, "axial", split_axis=0, concat_axis=2, tiled=True),
            lax.all_to_all(right_groups, "axial", split_axis=0, concat_axis=2, tiled=True),
        )
    )
    restored = lax.all_to_all(product, "axial", split_axis=2, concat_axis=0, tiled=True).reshape(
        channels, row_count, width
    )
    tri_norm = (normalize(restored.astype(jnp.float32), 0) * gain_vals[1][:, None, None]).astype(
        jnp.bfloat16
    )
    update = jnp.einsum("crn,cd->rnd", tri_norm, out_mat, preferred_element_type=jnp.float32)
    gate_values = jax.nn.sigmoid(
        jnp.einsum("rnd,dc->rnc", normed, proj_mats[4], preferred_element_type=jnp.float32)
    )
    pair_mid = pair_f + gate_values * update
    trans_in = (normalize(pair_mid, 2) * gain_vals[2]).astype(jnp.bfloat16).reshape(-1, channels)
    hidden = jax.nn.relu(jnp.dot(trans_in, up_mat, preferred_element_type=jnp.float32)).astype(
        jnp.bfloat16
    )
    pair_new = pair_mid + jnp.dot(hidden, down_mat, preferred_element_type=jnp.float32).reshape(
        pair_mid.shape
    )
    return pair_new.astype(jnp.bfloat16)


MESH = pl.DeviceIdType.MESH


def sigmoid(values):
    return 0.5 * jnp.tanh(0.5 * values) + 0.5


def normalize_rows(values, gain):
    scale = 1.0 / values.shape[0]
    center = values - jnp.sum(values, axis=0, keepdims=True) * scale
    spread = jnp.sum(center * center, axis=0, keepdims=True) * scale
    return center * lax.rsqrt(spread + epsilon) * gain


def matmul(mat, values):
    return lax.dot_general(mat, values, (((1,), (0,)), ((), ())), preferred_element_type=jnp.float32)


def fused_kernel(
    sections,
    ranks,
    halves,
    own_count,
    sub_rows,
    pair_ref,
    mask_ref,
    mask_smem,
    proj_ref,
    out_ref,
    up_ref,
    down_ref,
    gain_ref,
    result_ref,
    pair_buf,
    z_buf,
    normed_buf,
    gate_buf,
    edge_send,
    edge_recv,
    tri_send,
    tri_recv,
    left_f,
    right_f,
    tri_f,
    result_buf,
    proj_raw,
    out_raw,
    up_raw,
    down_raw,
    gain_all,
    proj_t,
    out_t,
    up_t,
    down_t,
    gain_t,
    pair_send_sem,
    pair_sem,
    edge_send_sem,
    edge_recv_sem,
    tri_send_sem,
    tri_recv_sem,
    result_send_sem,
    result_recv_sem,
    raw_sem,
    weight_send_sem,
    weight_pass_sem,
    weight_sem,
):
    section = lax.axis_index("section")
    axial = lax.axis_index("axial")
    span = ranks // sections
    group = axial // span
    place = lax.rem(axial, span)
    core = lax.rem(axial, 2)
    rank = section * span + place
    piece_rows, width, channels = pair_buf.shape[2:]
    rows = piece_rows * sections
    owners = ranks // halves
    per_group = channels // owners
    my_half = rank // owners
    my_owner = lax.rem(rank, owners)
    steps = piece_rows // sub_rows
    everyone = range(own_count)
    pieces = range(sections)

    def member(index):
        return {"section": index // span, "axial": group * span + lax.rem(index, span)}

    def part_of(t):
        return lax.rem(group + t, sections)

    def first_row(t, section_at, place_at):
        return (part_of(t) * span + place_at) * rows + section_at * piece_rows

    own_rows = pl.ds(section * piece_rows, piece_rows)

    for m in everyone:
        pltpu.make_async_copy(
            pair_ref.at[group * own_count + m, own_rows], pair_buf.at[m, 0], pair_sem.at[m, 0]
        ).start()
    raw_copies = [
        pltpu.make_async_copy(source, target, raw_sem.at[index])
        for index, (source, target) in enumerate(
            (
                (gain_ref.at[0], gain_all.at[section]),
                (proj_ref.at[0, pl.ds(2, 2)], proj_raw.at[pl.ds(2, 2)]),
                (proj_ref.at[0, pl.ds(0, 2)], proj_raw.at[pl.ds(0, 2)]),
                (proj_ref.at[0, pl.ds(4, 1)], proj_raw.at[pl.ds(4, 1)]),
                (out_ref.at[0], out_raw),
                (up_ref.at[0], up_raw),
                (down_ref.at[0], down_raw),
            )
        )
    ]
    for copy in raw_copies:
        copy.start()

    barrier = pltpu.get_barrier_semaphore()
    for k in range(1, ranks):
        pl.semaphore_signal(
            barrier, inc=1, device_id=member(lax.rem(rank + k, ranks)), device_id_type=MESH
        )
    for k in range(1, sections):
        for j in range(sections):
            pl.semaphore_signal(
                barrier,
                inc=1,
                device_id={
                    "section": lax.rem(section + j, sections),
                    "axial": part_of(k) * span + place,
                },
                device_id_type=MESH,
            )

    items = (
        (1, lambda layer: gain_all.at[layer]),
        (1, lambda layer: proj_t.at[layer, 2]),
        (1, lambda layer: proj_t.at[layer, 3]),
        (1, lambda layer: proj_t.at[layer, 0]),
        (1, lambda layer: proj_t.at[layer, 1]),
        (1, lambda layer: proj_t.at[layer, 4]),
        (1, lambda layer: out_t.at[layer]),
        (0, lambda layer: up_t.at[layer]),
        (0, lambda layer: down_t.at[layer]),
    )

    def item_copy(a, k):
        view = items[a][1](section)
        return pltpu.make_async_remote_copy(
            src_ref=view,
            dst_ref=view,
            send_sem=weight_send_sem.at[a, k],
            recv_sem=weight_sem.at[a, section],
            device_id={"section": lax.rem(section + k, sections)},
            device_id_type=MESH,
        )

    def item_pass(a, layer):
        view = items[a][1](layer)
        return pltpu.make_async_remote_copy(
            src_ref=view,
            dst_ref=view,
            send_sem=weight_pass_sem.at[a, layer],
            recv_sem=weight_sem.at[a, layer],
            device_id={"axial": axial + 1 - 2 * core},
            device_id_type=MESH,
        )

    def send_items(chosen):
        for side in range(2):

            @pl.when(core == side)
            def start():
                for a in chosen:
                    if items[a][0] == side:
                        for k in range(1, sections):
                            item_copy(a, k).start()

    def wait_item(a, layer):
        view = items[a][1](layer)
        pltpu.make_async_copy(view, view, weight_sem.at[a, layer]).wait()

    def pass_items(chosen, layer):
        for side in range(2):

            @pl.when(core == side)
            def give_on():
                for a in chosen:
                    if items[a][0] == side:
                        wait_item(a, layer)
                        item_pass(a, layer).start()

    def wait_items(chosen, layer):
        for side in range(2):

            @pl.when(core == side)
            def receive():
                for a in chosen:
                    if items[a][0] != side:
                        wait_item(a, layer)

    def finish_items():
        for side in range(2):

            @pl.when(core == side)
            def finish():
                for a, (owner, _) in enumerate(items):
                    if owner == side:
                        for k in range(1, sections):
                            item_copy(a, k).wait_send()
                        for k in range(1, sections):
                            item_pass(a, lax.rem(section + k, sections)).wait_send()

    def turned(values):
        return values.astype(jnp.float32).T.astype(jnp.bfloat16)

    def prepare_gains(layer):
        for index in range(gain_t.shape[1]):
            row = gain_all[layer, index : index + 1, :].astype(jnp.float32)
            gain_t[layer, index] = jnp.broadcast_to(row, (width, channels)).T

    def prepare_edges():
        raw_copies[0].wait()
        for pair in (1, 0):
            raw_copies[2 - pair].wait()
            for e in (2 * pair, 2 * pair + 1):
                proj_t[section, e] = turned(proj_raw[e])

    def prepare_rest():
        raw_copies[3].wait()
        proj_t[section, 4] = turned(proj_raw[4])
        for copy in raw_copies[4:]:
            copy.wait()
        out_t[section] = turned(out_raw[...])
        up_t[section] = turned(up_raw[...])
        down_t[section] = turned(down_raw[...])

    def wide_gain(layer, index):
        return jnp.concatenate([gain_t[layer, index]] * sub_rows, axis=1)

    def pair_copy(m, k):
        target = part_of(k)
        return pltpu.make_async_remote_copy(
            src_ref=pair_ref.at[target * own_count + m, own_rows],
            dst_ref=pair_buf.at[m, sections - k],
            send_sem=pair_send_sem.at[m, k],
            recv_sem=pair_sem.at[m, sections - k],
            device_id={"axial": target * span + place},
            device_id_type=MESH,
        )

    def load_pair(m, t):
        pltpu.make_async_copy(pair_buf.at[m, t], pair_buf.at[m, t], pair_sem.at[m, t]).wait()
        for q in range(steps):
            for i in range(sub_rows):
                z_buf[m, t, q, :, i * width : (i + 1) * width] = (
                    pair_buf[m, t, q * sub_rows + i].astype(jnp.float32).T
                )

    def phase_norm(layer, m, t):
        for q in range(steps):
            normed_buf[m, t, q] = normalize_rows(z_buf[m, t, q], wide_gain(layer, 0)).astype(
                jnp.bfloat16
            )

    def phase_edges(layer, m, t):
        crop = group * own_count + m
        row_mask = mask_ref[pl.ds(crop, 1), :].astype(jnp.float32)
        start = first_row(t, section, place)
        for q in range(steps):
            values = normed_buf[m, t, q]
            masks = []
            for i in range(sub_rows):
                own = mask_smem[crop, start + q * sub_rows + i]
                masks.append(row_mask * own.astype(jnp.float32))
            pair_mask = jnp.concatenate(masks, axis=1)
            for side in (1, 0):
                value = matmul(proj_t[layer, 2 * side], values)
                gate = matmul(proj_t[layer, 2 * side + 1], values)
                edge = sigmoid(gate) * value * pair_mask
                for i in range(sub_rows):
                    part = edge[:, i * width : (i + 1) * width].reshape(owners, per_group, width)
                    edge_send[m, t, :, side, q * sub_rows + i] = part.astype(jnp.bfloat16)

    def phase_gate(layer, m, t):
        for q in range(steps):
            gate_buf[m, t, q] = sigmoid(matmul(proj_t[layer, 4], normed_buf[m, t, q]))

    def rank_at(half_step, index):
        if halves == 1:
            return index
        return lax.rem(my_half + half_step, halves) * owners + index

    def edge_view(ref, half_step):
        return ref if half_step == 0 else ref.at[1]

    def edge_copy(slot, m, t, k):
        half_step = k // owners
        owner = lax.rem(my_owner + k % owners, owners)
        return pltpu.make_async_remote_copy(
            src_ref=edge_view(edge_send.at[m, t, owner], half_step),
            dst_ref=edge_view(edge_recv.at[slot, m, t, rank], half_step),
            send_sem=edge_send_sem.at[m, t],
            recv_sem=edge_recv_sem.at[slot, m, t],
            device_id=member(rank_at(half_step, owner)),
            device_id_type=MESH,
        )

    def send_edges(slot, m, t):
        for k in range(ranks - 1, 0, -1):
            edge_copy(slot, m, t, k).start()
        pltpu.make_async_copy(
            edge_send.at[m, t, my_owner],
            edge_recv.at[slot, m, t, rank],
            edge_recv_sem.at[slot, m, t],
        ).start()

    def wait_edges_sent(m, t):
        left_over = (halves - 1) * owners
        sent = edge_recv.at[0, m, t, pl.ds(0, owners - 1 + left_over // 2)]
        pltpu.make_async_copy(sent, sent, edge_send_sem.at[m, t]).wait()

    def wait_edges(slot, m, t):
        left_over = (halves - 1) * owners
        got = edge_recv.at[slot, m, t, pl.ds(0, owners + left_over // 2)]
        pltpu.make_async_copy(got, got, edge_recv_sem.at[slot, m, t]).wait()

    def tri_copy(m, t, k):
        owner = lax.rem(my_owner + k, owners)
        return pltpu.make_async_remote_copy(
            src_ref=tri_send.at[m, t, owner],
            dst_ref=tri_recv.at[m, t, my_owner],
            send_sem=tri_send_sem.at[m, t],
            recv_sem=tri_recv_sem.at[m, t],
            device_id=member(my_half * owners + owner),
            device_id_type=MESH,
        )

    def send_tri(m, t):
        for k in range(owners - 1, 0, -1):
            tri_copy(m, t, k).start()
        pltpu.make_async_copy(
            tri_send.at[m, t, my_owner], tri_recv.at[m, t, my_owner], tri_recv_sem.at[m, t]
        ).start()

    def wait_tri_sent(m):
        for t in pieces:
            sent = tri_recv.at[m, t, pl.ds(0, owners - 1)]
            pltpu.make_async_copy(sent, sent, tri_send_sem.at[m, t]).wait()

    def wait_tri(m, t):
        pltpu.make_async_copy(tri_recv.at[m, t], tri_recv.at[m, t], tri_recv_sem.at[m, t]).wait()

    def phase_triangle(slot, m, order):
        columns = [slice(w * 128, (w + 1) * 128) for w in range(width // 128)]
        piece_lines = piece_rows * per_group

        def spread(target, at, values):
            for w, lanes in enumerate(columns):
                target[w, pl.ds(at, piece_lines)] = (
                    values[:, :, lanes].astype(jnp.float32).reshape(piece_lines, 128)
                )

        def channel(source, c, count):
            lines = pl.ds(c, count, stride=per_group)
            return jnp.concatenate(
                [source[w, lines, :].astype(jnp.bfloat16) for w in range(len(columns))], axis=1
            )

        for t in pieces:
            wait_edges(slot, m, t)
            for half_step in range(halves):
                for index in range(owners):
                    g = rank_at(half_step, index)
                    start = first_row(t, g // span, g % span if halves == 1 else lax.rem(g, span))
                    spread(
                        right_f,
                        pl.multiple_of(start * per_group, 8),
                        edge_recv[slot, m, t, g, 1],
                    )
                    if half_step == 0:
                        at = index * rows + t * piece_rows
                        spread(left_f, at * per_group, edge_recv[slot, m, t, g, 0])
        for c in range(per_group):
            product = lax.dot_general(
                channel(left_f, c, owners * rows),
                channel(right_f, c, ranks * rows),
                (((1,), (1,)), ((), ())),
                preferred_element_type=jnp.float32,
            )
            for w, lanes in enumerate(columns):
                tri_f[w, pl.ds(c, owners * rows, stride=per_group), :] = product[:, lanes]
        for t in order:
            for g in range(owners):
                at = (g * rows + t * piece_rows) * per_group
                for w, lanes in enumerate(columns):
                    part = tri_f[w, at : at + piece_lines].reshape(piece_rows, per_group, 128)
                    tri_send[m, t, g, :, :, lanes] = part.astype(jnp.bfloat16)
            send_tri(m, t)

    def phase_update(layer, m, t, last):
        span_q = range(steps)

        def tri_at(q):
            parts = []
            for i in range(sub_rows):
                part = tri_recv[m, t, :, q * sub_rows + i].astype(jnp.float32)
                parts.append(part.reshape(channels, width))
            return jnp.concatenate(parts, axis=1)

        gain_tri, gain_in = wide_gain(layer, 1), wide_gain(layer, 2)
        tri_norm = [normalize_rows(tri_at(q), gain_tri).astype(jnp.bfloat16) for q in span_q]
        update = [matmul(out_t[layer], tri_norm[q]) for q in span_q]
        mid = [z_buf[m, t, q] + gate_buf[m, t, q] * update[q] for q in span_q]
        trans_in = [normalize_rows(mid[q], gain_in).astype(jnp.bfloat16) for q in span_q]
        hidden = [
            jnp.maximum(matmul(up_t[layer], trans_in[q]), 0.0).astype(jnp.bfloat16) for q in span_q
        ]
        fresh = [mid[q] + matmul(down_t[layer], hidden[q]) for q in span_q]
        for q in span_q:
            if last:
                for i in range(sub_rows):
                    part = fresh[q][:, i * width : (i + 1) * width]
                    result_buf[m, t, q * sub_rows + i] = part.T.astype(jnp.bfloat16)
            else:
                z_buf[m, t, q] = fresh[q].astype(jnp.bfloat16).astype(jnp.float32)

    def result_copy(m, t):
        return pltpu.make_async_remote_copy(
            src_ref=result_buf.at[m, t],
            dst_ref=result_ref.at[m, own_rows],
            send_sem=result_send_sem.at[m, t],
            recv_sem=result_recv_sem.at[m, section],
            device_id={"section": group, "axial": part_of(t) * span + place},
            device_id_type=MESH,
        )

    def send_result(m, t):
        if t > 0:
            result_copy(m, t).start()
            return

        @pl.when(section == group)
        def keep():
            pltpu.make_async_copy(
                result_buf.at[m, t], result_ref.at[m, own_rows], result_recv_sem.at[m, section]
            ).start()

        @pl.when(section != group)
        def give():
            result_copy(m, t).start()

    def finish_results():
        for m in everyone:
            for t in pieces:
                if t > 0:
                    result_copy(m, t).wait_send()
                else:

                    @pl.when(section != group)
                    def given():
                        result_copy(m, t).wait_send()

            for s in range(sections):
                part = result_ref.at[m, pl.ds(s * piece_rows, piece_rows)]
                pltpu.make_async_copy(part, part, result_recv_sem.at[m, s]).wait()

    edge_items = range(5)
    rest_items = range(5, len(items))
    prepare_edges()
    pl.semaphore_wait(barrier, ranks - 1 + (sections - 1) * sections)

    @pl.when(section == 0)
    def first_items():
        send_items(edge_items)

    for k in range(1, sections):
        pair_copy(0, k).start()
    prepare_gains(section)

    @pl.when(section != 0)
    def other_items():
        prepare_rest()
        send_items(range(len(items)))

    for m in everyone:
        load_pair(m, 0)

    @pl.when(section != 0)
    def first_weights():
        pass_items(edge_items, 0)
        wait_items(edge_items, 0)
        prepare_gains(0)

    phase_norm(0, 0, 0)
    phase_edges(0, 0, 0)
    send_edges(0, 0, 0)
    for m in everyone[1:]:
        for k in range(1, sections):
            pair_copy(m, k).start()

    @pl.when(section == 0)
    def second_items():
        prepare_rest()
        send_items(rest_items)

    for m in everyone[1:]:
        phase_norm(0, m, 0)
        phase_edges(0, m, 0)
    for other in range(1, sections):

        @pl.when(section != other)
        def relay_later():
            pass_items(range(len(items)), other)

    for m in everyone:
        for t in pieces[1:]:
            load_pair(m, t)
            phase_norm(0, m, t)
            phase_edges(0, m, t)
            send_edges(0, m, t)
        if m == 0:

            @pl.when(section != 0)
            def relay_first():
                pass_items(rest_items, 0)

        if m + 1 < own_count:
            send_edges(0, m + 1, 0)

    @pl.when(section != 0)
    def other_weights():
        wait_items(rest_items, 0)

    for m in everyone:
        for t in pieces:
            phase_gate(0, m, t)

    for layer in range(sections):
        last = layer == sections - 1
        order = pieces[::-1] if last else pieces
        for m in everyone:
            if layer > 0:
                wait_tri_sent(m)
            phase_triangle(layer % 2, m, order)
        if layer == 0:
            for other in range(1, sections):

                @pl.when(section != other)
                def later_weights():
                    wait_items(range(len(items)), other)
                    prepare_gains(other)

        for m in everyone:
            for t in order:
                wait_tri(m, t)
                phase_update(layer, m, t, last)
                wait_edges_sent(m, t)
                if last:
                    send_result(m, t)
                else:
                    phase_norm(layer + 1, m, t)
                    phase_edges(layer + 1, m, t)
                    send_edges((layer + 1) % 2, m, t)
        if not last:
            for m in everyone:
                for t in pieces:
                    phase_gate(layer + 1, m, t)
    for m in everyone:
        wait_tri_sent(m)
        for k in range(1, sections):
            pair_copy(m, k).wait_send()
    finish_items()
    finish_results()


def fused_device(pair_in, crop_mask, proj_weights, out_weights, up_weights, down_weights, norm_gains):
    sections = lax.axis_size("section")
    ranks = lax.axis_size("axial")
    micro_count, rows, width, channels = pair_in.shape
    own_count = micro_count // sections
    halves = half_count(pair_in)
    owners = ranks // halves
    per_group = channels // owners
    piece_rows = rows // sections
    sub_rows = 2 if piece_rows % 2 == 0 else 1
    steps = piece_rows // sub_rows
    lanes = sub_rows * width
    hidden = up_weights.shape[2]
    gains = norm_gains.shape[1]
    edge_kinds = proj_weights.shape[1]
    bf16, f32 = jnp.bfloat16, jnp.float32
    vmem = pl.BlockSpec(memory_space=pltpu.VMEM)
    hbm = pl.BlockSpec(memory_space=pltpu.HBM)
    dma = pltpu.SemaphoreType.DMA
    piece = (piece_rows, per_group, width)
    rows_shape = (own_count, sections, piece_rows, width, channels)
    wide_shape = (own_count, sections, steps, channels, lanes)
    tri_shape = (own_count, sections, owners) + piece
    return pl.pallas_call(
        functools.partial(fused_kernel, sections, ranks, halves, own_count, sub_rows),
        out_shape=pltpu.VMEM((own_count, rows, width, channels), bf16),
        in_specs=[hbm, vmem, pl.BlockSpec(memory_space=pltpu.SMEM)] + [hbm] * 5,
        out_specs=vmem,
        scratch_shapes=[
            pltpu.VMEM(rows_shape, bf16),
            pltpu.VMEM(wide_shape, f32),
            pltpu.VMEM(wide_shape, bf16),
            pltpu.VMEM(wide_shape, f32),
            pltpu.VMEM((own_count, sections, owners, 2) + piece, bf16),
            pltpu.VMEM((2, own_count, sections, ranks, 2) + piece, bf16),
            pltpu.VMEM(tri_shape, bf16),
            pltpu.VMEM(tri_shape, bf16),
            pltpu.VMEM((width // 128, owners * rows * per_group, 128), f32),
            pltpu.VMEM((width // 128, ranks * rows * per_group, 128), f32),
            pltpu.VMEM((width // 128, owners * rows * per_group, 128), f32),
            pltpu.VMEM(rows_shape, bf16),
            pltpu.VMEM(proj_weights.shape[1:], bf16),
            pltpu.VMEM(out_weights.shape[1:], bf16),
            pltpu.VMEM(up_weights.shape[1:], bf16),
            pltpu.VMEM(down_weights.shape[1:], bf16),
            pltpu.VMEM((sections,) + norm_gains.shape[1:], bf16),
            pltpu.VMEM((sections, edge_kinds, channels, channels), bf16),
            pltpu.VMEM((sections, channels, channels), bf16),
            pltpu.VMEM((sections, hidden, channels), bf16),
            pltpu.VMEM((sections, channels, hidden), bf16),
            pltpu.VMEM((sections, gains, channels, width), f32),
            dma((own_count, sections)),
            dma((own_count, sections)),
            dma((own_count, sections)),
            dma((2, own_count, sections)),
            dma((own_count, sections)),
            dma((own_count, sections)),
            dma((own_count, sections)),
            dma((own_count, sections)),
            dma((7,)),
            dma((9, sections)),
            dma((9, sections)),
            dma((9, sections)),
        ],
        compiler_params=pltpu.CompilerParams(
            collective_id=0, has_side_effects=True, vmem_limit_bytes=67043328 - 2 * own_count * rows * width * channels
        ),
    )(
        pair_in,
        crop_mask,
        crop_mask,
        proj_weights,
        out_weights,
        up_weights,
        down_weights,
        norm_gains,
    )


def half_count(pair_in):
    ranks = lax.axis_size("axial")
    return 2 if ranks % 2 == 0 and pair_in.shape[3] % (8 * ranks) else 1


def fits_fused(pair_in):
    rows, width, channels = pair_in.shape[1:]
    sections = lax.axis_size("section")
    ranks = lax.axis_size("axial")
    owners = ranks // half_count(pair_in)
    return (
        channels % (8 * owners) == 0
        and rows % sections == 0
        and width % 128 == 0
        and ranks % (2 * sections) == 0
    )


def per_device(pair_in, crop_mask, proj_weights, out_weights, up_weights, down_weights, norm_gains):
    if fits_fused(pair_in):
        return fused_device(
            pair_in, crop_mask, proj_weights, out_weights, up_weights, down_weights, norm_gains
        )
    section_index = lax.axis_index("section")
    section_count = lax.axis_size("section")
    micro_count = pair_in.shape[0]
    own_count = micro_count // section_count
    gathered = (
        lax.all_gather(proj_weights, "section", axis=0, tiled=True),
        lax.all_gather(out_weights, "section", axis=0, tiled=True),
        lax.all_gather(up_weights, "section", axis=0, tiled=True),
        lax.all_gather(down_weights, "section", axis=0, tiled=True),
        lax.all_gather(norm_gains, "section", axis=0, tiled=True),
    )
    own_pairs = lax.dynamic_slice_in_dim(pair_in, section_index * own_count, own_count, 0)
    own_masks = lax.dynamic_slice_in_dim(crop_mask, section_index * own_count, own_count, 0).astype(
        jnp.float32
    )
    outputs = []
    for member in range(own_count):
        current = own_pairs[member]
        for layer_index in range(section_count):
            current = evo_block(
                current,
                own_masks[member],
                gathered[0][layer_index],
                gathered[1][layer_index],
                gathered[2][layer_index],
                gathered[3][layer_index],
                gathered[4][layer_index],
            )
        outputs.append(current)
    return jnp.stack(outputs)


def solution(mesh):
    return jax.shard_map(
        per_device,
        mesh=mesh,
        in_specs=(
            P("groups", "axial", None, None),
            P("groups", None),
            P("section", None, None, None),
            P("section", None, None),
            P("section", None, None),
            P("section", None, None),
            P("section", None, None),
        ),
        out_specs=P(("groups", "section"), "axial", None, None),
        check_vma=False,
    )
```

```python
import functools

import jax
import jax.numpy as jnp
from jax import lax
from jax.experimental import pallas as pl
from jax.experimental.pallas import tpu as pltpu
from jax.sharding import PartitionSpec as P

epsilon = 1e-05


def normalize(values, axis_dim):
    center = values - jnp.mean(values, axis=axis_dim, keepdims=True)
    spread = jnp.mean(center * center, axis=axis_dim, keepdims=True)
    return center * lax.rsqrt(spread + epsilon)


def triangle(pieces):
    return jnp.einsum(
        "gcik,gcjk->gcij", pieces[0], pieces[1], preferred_element_type=jnp.float32
    ).astype(jnp.bfloat16)


def evo_block(current, mask_all, proj_mats, out_mat, up_mat, down_mat, gain_rows):
    row_count = current.shape[0]
    width = current.shape[1]
    channels = current.shape[2]
    group_count = lax.axis_size("axial")
    per_group = channels // group_count
    row_start = lax.axis_index("axial") * row_count
    mask_rows = lax.dynamic_slice_in_dim(mask_all, row_start, row_count)
    gain_vals = gain_rows.astype(jnp.float32)
    pair_f = current.astype(jnp.float32)
    normed = (normalize(pair_f, 2) * gain_vals[0]).astype(jnp.bfloat16)
    linear = jnp.einsum("rnd,edc->ecrn", normed, proj_mats[:4], preferred_element_type=jnp.float32)
    pair_mask = mask_rows[:, None] * mask_all[None, :]
    left_edge = (jax.nn.sigmoid(linear[1]) * linear[0] * pair_mask).astype(jnp.bfloat16)
    right_edge = (jax.nn.sigmoid(linear[3]) * linear[2] * pair_mask).astype(jnp.bfloat16)
    left_groups = left_edge.reshape(group_count, per_group, row_count, width)
    right_groups = right_edge.reshape(group_count, per_group, row_count, width)
    product = triangle(
        (
            lax.all_to_all(left_groups, "axial", split_axis=0, concat_axis=2, tiled=True),
            lax.all_to_all(right_groups, "axial", split_axis=0, concat_axis=2, tiled=True),
        )
    )
    restored = lax.all_to_all(product, "axial", split_axis=2, concat_axis=0, tiled=True).reshape(
        channels, row_count, width
    )
    tri_norm = (normalize(restored.astype(jnp.float32), 0) * gain_vals[1][:, None, None]).astype(
        jnp.bfloat16
    )
    update = jnp.einsum("crn,cd->rnd", tri_norm, out_mat, preferred_element_type=jnp.float32)
    gate_values = jax.nn.sigmoid(
        jnp.einsum("rnd,dc->rnc", normed, proj_mats[4], preferred_element_type=jnp.float32)
    )
    pair_mid = pair_f + gate_values * update
    trans_in = (normalize(pair_mid, 2) * gain_vals[2]).astype(jnp.bfloat16).reshape(-1, channels)
    hidden = jax.nn.relu(jnp.dot(trans_in, up_mat, preferred_element_type=jnp.float32)).astype(
        jnp.bfloat16
    )
    pair_new = pair_mid + jnp.dot(hidden, down_mat, preferred_element_type=jnp.float32).reshape(
        pair_mid.shape
    )
    return pair_new.astype(jnp.bfloat16)


MESH = pl.DeviceIdType.MESH


def sigmoid(values):
    return 0.5 * jnp.tanh(0.5 * values) + 0.5


def normalize_rows(values, gain):
    scale = 1.0 / values.shape[0]
    center = values - jnp.sum(values, axis=0, keepdims=True) * scale
    spread = jnp.sum(center * center, axis=0, keepdims=True) * scale
    return center * lax.rsqrt(spread + epsilon) * gain


def matmul(mat, values):
    return lax.dot_general(mat, values, (((1,), (0,)), ((), ())), preferred_element_type=jnp.float32)


def fused_kernel(
    sections,
    ranks,
    halves,
    own_count,
    sub_rows,
    pair_ref,
    mask_ref,
    mask_smem,
    proj_ref,
    out_ref,
    up_ref,
    down_ref,
    gain_ref,
    result_ref,
    pair_buf,
    pair_stage,
    z_buf,
    normed_buf,
    gate_buf,
    edge_send,
    edge_recv,
    tri_send,
    tri_recv,
    left_f,
    right_f,
    tri_f,
    result_buf,
    proj_raw,
    out_raw,
    up_raw,
    down_raw,
    gain_all,
    proj_t,
    out_t,
    up_t,
    down_t,
    gain_t,
    pair_stage_sem,
    pair_send_sem,
    pair_sem,
    edge_send_sem,
    edge_recv_sem,
    tri_send_sem,
    tri_recv_sem,
    result_send_sem,
    result_recv_sem,
    raw_sem,
    weight_send_sem,
    weight_pass_sem,
    weight_sem,
):
    section = lax.axis_index("section")
    axial = lax.axis_index("axial")
    span = ranks // sections
    group = axial // span
    place = lax.rem(axial, span)
    core = lax.rem(axial, 2)
    rank = section * span + place
    piece_rows, width, channels = pair_buf.shape[2:]
    rows = piece_rows * sections
    owners = ranks // halves
    per_group = channels // owners
    my_half = rank // owners
    my_owner = lax.rem(rank, owners)
    steps = piece_rows // sub_rows
    everyone = range(own_count)
    pieces = range(sections)

    def member(index):
        return {"section": index // span, "axial": group * span + lax.rem(index, span)}

    def part_of(t):
        return lax.rem(group + t, sections)

    def first_row(t, section_at, place_at):
        return (part_of(t) * span + place_at) * rows + section_at * piece_rows

    own_rows = pl.ds(section * piece_rows, piece_rows)

    barrier = pltpu.get_barrier_semaphore()
    for k in range(1, ranks):
        pl.semaphore_signal(
            barrier, inc=1, device_id=member(lax.rem(rank + k, ranks)), device_id_type=MESH
        )
    for k in range(1, sections):
        for j in range(sections):
            pl.semaphore_signal(
                barrier,
                inc=1,
                device_id={
                    "section": lax.rem(section + j, sections),
                    "axial": part_of(k) * span + place,
                },
                device_id_type=MESH,
            )

    def stage_copy(m, k):
        return pltpu.make_async_copy(
            pair_ref.at[part_of(k) * own_count + m, own_rows],
            pair_stage.at[m, k - 1],
            pair_stage_sem.at[m, k - 1],
        )

    for m in everyone:
        pltpu.make_async_copy(
            pair_ref.at[group * own_count + m, own_rows], pair_buf.at[m, 0], pair_sem.at[m, 0]
        ).start()
    for m in everyone:
        for k in range(1, sections):
            stage_copy(m, k).start()
    raw_copies = [
        pltpu.make_async_copy(source, target, raw_sem.at[index])
        for index, (source, target) in enumerate(
            (
                (gain_ref.at[0], gain_all.at[section]),
                (proj_ref.at[0, pl.ds(2, 2)], proj_raw.at[pl.ds(2, 2)]),
                (proj_ref.at[0, pl.ds(0, 2)], proj_raw.at[pl.ds(0, 2)]),
                (proj_ref.at[0, pl.ds(4, 1)], proj_raw.at[pl.ds(4, 1)]),
                (out_ref.at[0], out_raw),
                (up_ref.at[0], up_raw),
                (down_ref.at[0], down_raw),
            )
        )
    ]
    for copy in raw_copies:
        copy.start()

    items = (
        (1, lambda layer: gain_all.at[layer]),
        (1, lambda layer: proj_t.at[layer, 2]),
        (1, lambda layer: proj_t.at[layer, 3]),
        (1, lambda layer: proj_t.at[layer, 0]),
        (1, lambda layer: proj_t.at[layer, 1]),
        (1, lambda layer: proj_t.at[layer, 4]),
        (1, lambda layer: out_t.at[layer]),
        (0, lambda layer: up_t.at[layer]),
        (0, lambda layer: down_t.at[layer]),
    )

    def item_copy(a, k):
        view = items[a][1](section)
        return pltpu.make_async_remote_copy(
            src_ref=view,
            dst_ref=view,
            send_sem=weight_send_sem.at[a, k],
            recv_sem=weight_sem.at[a, section],
            device_id={"section": lax.rem(section + k, sections)},
            device_id_type=MESH,
        )

    def item_pass(a, layer):
        view = items[a][1](layer)
        return pltpu.make_async_remote_copy(
            src_ref=view,
            dst_ref=view,
            send_sem=weight_pass_sem.at[a, layer],
            recv_sem=weight_sem.at[a, layer],
            device_id={"axial": axial + 1 - 2 * core},
            device_id_type=MESH,
        )

    def send_items(chosen):
        for side in range(2):

            @pl.when(core == side)
            def start():
                for a in chosen:
                    if items[a][0] == side:
                        for k in range(1, sections):
                            item_copy(a, k).start()

    def wait_item(a, layer):
        view = items[a][1](layer)
        pltpu.make_async_copy(view, view, weight_sem.at[a, layer]).wait()

    def pass_items(chosen, layer):
        for side in range(2):

            @pl.when(core == side)
            def give_on():
                for a in chosen:
                    if items[a][0] == side:
                        wait_item(a, layer)
                        item_pass(a, layer).start()

    def wait_items(chosen, layer):
        for side in range(2):

            @pl.when(core == side)
            def receive():
                for a in chosen:
                    if items[a][0] != side:
                        wait_item(a, layer)

    def finish_items():
        for side in range(2):

            @pl.when(core == side)
            def finish():
                for a, (owner, _) in enumerate(items):
                    if owner == side:
                        for k in range(1, sections):
                            item_copy(a, k).wait_send()
                        for k in range(1, sections):
                            item_pass(a, lax.rem(section + k, sections)).wait_send()

    def turned(values):
        return values.astype(jnp.float32).T.astype(jnp.bfloat16)

    def prepare_gains(layer):
        for index in range(gain_t.shape[1]):
            row = gain_all[layer, index : index + 1, :].astype(jnp.float32)
            gain_t[layer, index] = jnp.broadcast_to(row, (width, channels)).T

    def prepare_edges():
        raw_copies[0].wait()
        for pair in (1, 0):
            raw_copies[2 - pair].wait()
            for e in (2 * pair, 2 * pair + 1):
                proj_t[section, e] = turned(proj_raw[e])

    def prepare_rest():
        raw_copies[3].wait()
        proj_t[section, 4] = turned(proj_raw[4])
        for copy in raw_copies[4:]:
            copy.wait()
        out_t[section] = turned(out_raw[...])
        up_t[section] = turned(up_raw[...])
        down_t[section] = turned(down_raw[...])

    def wide_gain(layer, index):
        return jnp.concatenate([gain_t[layer, index]] * sub_rows, axis=1)

    def pair_copy(m, k):
        target = part_of(k)
        return pltpu.make_async_remote_copy(
            src_ref=pair_stage.at[m, k - 1],
            dst_ref=pair_buf.at[m, sections - k],
            send_sem=pair_send_sem.at[m, k],
            recv_sem=pair_sem.at[m, sections - k],
            device_id={"axial": target * span + place},
            device_id_type=MESH,
        )

    def load_pair(m, t):
        pltpu.make_async_copy(pair_buf.at[m, t], pair_buf.at[m, t], pair_sem.at[m, t]).wait()
        for q in range(steps):
            for i in range(sub_rows):
                z_buf[m, t, q, :, i * width : (i + 1) * width] = (
                    pair_buf[m, t, q * sub_rows + i].astype(jnp.float32).T
                )

    def phase_norm(layer, m, t):
        for q in range(steps):
            normed_buf[m, t, q] = normalize_rows(z_buf[m, t, q], wide_gain(layer, 0)).astype(
                jnp.bfloat16
            )

    def phase_edges(layer, m, t):
        crop = group * own_count + m
        row_mask = mask_ref[pl.ds(crop, 1), :].astype(jnp.float32)
        start = first_row(t, section, place)
        for q in range(steps):
            values = normed_buf[m, t, q]
            masks = []
            for i in range(sub_rows):
                own = mask_smem[crop, start + q * sub_rows + i]
                masks.append(row_mask * own.astype(jnp.float32))
            pair_mask = jnp.concatenate(masks, axis=1)
            for side in (1, 0):
                value = matmul(proj_t[layer, 2 * side], values)
                gate = matmul(proj_t[layer, 2 * side + 1], values)
                edge = sigmoid(gate) * value * pair_mask
                for i in range(sub_rows):
                    part = edge[:, i * width : (i + 1) * width].reshape(owners, per_group, width)
                    edge_send[m, t, :, side, q * sub_rows + i] = part.astype(jnp.bfloat16)

    def phase_gate(layer, m, t):
        for q in range(steps):
            gate_buf[m, t, q] = sigmoid(matmul(proj_t[layer, 4], normed_buf[m, t, q]))

    def rank_at(half_step, index):
        if halves == 1:
            return index
        return lax.rem(my_half + half_step, halves) * owners + index

    def partner(k):
        if owners & (owners - 1):
            return lax.rem(my_owner + k, owners)
        index, unit = 0, 1
        while unit < owners:
            bit = lax.rem(my_owner // unit, 2)
            index += unit * (1 - bit if k // unit % 2 else bit)
            unit *= 2
        return index

    def edge_view(ref, half_step):
        return ref if half_step == 0 else ref.at[1]

    def edge_copy(slot, m, t, k):
        half_step = k // owners
        owner = partner(k % owners)
        return pltpu.make_async_remote_copy(
            src_ref=edge_view(edge_send.at[m, t, owner], half_step),
            dst_ref=edge_view(edge_recv.at[slot, m, t, rank], half_step),
            send_sem=edge_send_sem.at[m, t],
            recv_sem=edge_recv_sem.at[slot, m, t],
            device_id=member(rank_at(half_step, owner)),
            device_id_type=MESH,
        )

    def send_edges(slot, m, t):
        for k in range(ranks - 1, 0, -1):
            edge_copy(slot, m, t, k).start()
        pltpu.make_async_copy(
            edge_send.at[m, t, my_owner],
            edge_recv.at[slot, m, t, rank],
            edge_recv_sem.at[slot, m, t],
        ).start()

    def wait_edges_sent(m, t):
        left_over = (halves - 1) * owners
        sent = edge_recv.at[0, m, t, pl.ds(0, owners - 1 + left_over // 2)]
        pltpu.make_async_copy(sent, sent, edge_send_sem.at[m, t]).wait()

    def wait_edges(slot, m, t):
        left_over = (halves - 1) * owners
        got = edge_recv.at[slot, m, t, pl.ds(0, owners + left_over // 2)]
        pltpu.make_async_copy(got, got, edge_recv_sem.at[slot, m, t]).wait()

    def tri_copy(m, t, k):
        owner = partner(k)
        return pltpu.make_async_remote_copy(
            src_ref=tri_send.at[m, t, owner],
            dst_ref=tri_recv.at[m, t, my_owner],
            send_sem=tri_send_sem.at[m, t],
            recv_sem=tri_recv_sem.at[m, t],
            device_id=member(my_half * owners + owner),
            device_id_type=MESH,
        )

    def send_tri(m, t):
        for k in range(owners - 1, 0, -1):
            tri_copy(m, t, k).start()
        pltpu.make_async_copy(
            tri_send.at[m, t, my_owner], tri_recv.at[m, t, my_owner], tri_recv_sem.at[m, t]
        ).start()

    def wait_tri_sent(m):
        for t in pieces:
            sent = tri_recv.at[m, t, pl.ds(0, owners - 1)]
            pltpu.make_async_copy(sent, sent, tri_send_sem.at[m, t]).wait()

    def wait_tri(m, t):
        pltpu.make_async_copy(tri_recv.at[m, t], tri_recv.at[m, t], tri_recv_sem.at[m, t]).wait()

    def phase_triangle(slot, m, order):
        columns = [slice(w * 128, (w + 1) * 128) for w in range(width // 128)]
        piece_lines = piece_rows * per_group

        def spread(target, at, values):
            for w, lanes in enumerate(columns):
                target[w, pl.ds(at, piece_lines)] = (
                    values[:, :, lanes].astype(jnp.float32).reshape(piece_lines, 128)
                )

        def channel(source, c, count):
            lines = pl.ds(c, count, stride=per_group)
            return jnp.concatenate(
                [source[w, lines, :].astype(jnp.bfloat16) for w in range(len(columns))], axis=1
            )

        for t in pieces:
            wait_edges(slot, m, t)
            for half_step in range(halves):
                for index in range(owners):
                    g = rank_at(half_step, index)
                    start = first_row(t, g // span, g % span if halves == 1 else lax.rem(g, span))
                    spread(
                        right_f,
                        pl.multiple_of(start * per_group, 8),
                        edge_recv[slot, m, t, g, 1],
                    )
                    if half_step == 0:
                        at = index * rows + t * piece_rows
                        spread(left_f, at * per_group, edge_recv[slot, m, t, g, 0])
        for c in range(per_group):
            product = lax.dot_general(
                channel(left_f, c, owners * rows),
                channel(right_f, c, ranks * rows),
                (((1,), (1,)), ((), ())),
                preferred_element_type=jnp.float32,
            )
            for w, lanes in enumerate(columns):
                tri_f[w, pl.ds(c, owners * rows, stride=per_group), :] = product[:, lanes]
        for t in order:
            for g in range(owners):
                at = (g * rows + t * piece_rows) * per_group
                for w, lanes in enumerate(columns):
                    part = tri_f[w, at : at + piece_lines].reshape(piece_rows, per_group, 128)
                    tri_send[m, t, g, :, :, lanes] = part.astype(jnp.bfloat16)
            send_tri(m, t)

    def phase_update(layer, m, t, last):
        span_q = range(steps)

        def tri_at(q):
            parts = []
            for i in range(sub_rows):
                part = tri_recv[m, t, :, q * sub_rows + i].astype(jnp.float32)
                parts.append(part.reshape(channels, width))
            return jnp.concatenate(parts, axis=1)

        gain_tri, gain_in = wide_gain(layer, 1), wide_gain(layer, 2)
        tri_norm = [normalize_rows(tri_at(q), gain_tri).astype(jnp.bfloat16) for q in span_q]
        update = [matmul(out_t[layer], tri_norm[q]) for q in span_q]
        mid = [z_buf[m, t, q] + gate_buf[m, t, q] * update[q] for q in span_q]
        trans_in = [normalize_rows(mid[q], gain_in).astype(jnp.bfloat16) for q in span_q]
        hidden = [
            jnp.maximum(matmul(up_t[layer], trans_in[q]), 0.0).astype(jnp.bfloat16) for q in span_q
        ]
        fresh = [mid[q] + matmul(down_t[layer], hidden[q]) for q in span_q]
        for q in span_q:
            if last:
                for i in range(sub_rows):
                    part = fresh[q][:, i * width : (i + 1) * width]
                    result_buf[m, t, q * sub_rows + i] = part.T.astype(jnp.bfloat16)
            else:
                z_buf[m, t, q] = fresh[q].astype(jnp.bfloat16).astype(jnp.float32)

    def result_copy(m, t):
        return pltpu.make_async_remote_copy(
            src_ref=result_buf.at[m, t],
            dst_ref=result_ref.at[m, own_rows],
            send_sem=result_send_sem.at[m, t],
            recv_sem=result_recv_sem.at[m, section],
            device_id={"section": group, "axial": part_of(t) * span + place},
            device_id_type=MESH,
        )

    def send_result(m, t):
        if t > 0:
            result_copy(m, t).start()
            return

        @pl.when(section == group)
        def keep():
            pltpu.make_async_copy(
                result_buf.at[m, t], result_ref.at[m, own_rows], result_recv_sem.at[m, section]
            ).start()

        @pl.when(section != group)
        def give():
            result_copy(m, t).start()

    def finish_results():
        for m in everyone:
            for t in pieces:
                if t > 0:
                    result_copy(m, t).wait_send()
                else:

                    @pl.when(section != group)
                    def given():
                        result_copy(m, t).wait_send()

            for s in range(sections):
                part = result_ref.at[m, pl.ds(s * piece_rows, piece_rows)]
                pltpu.make_async_copy(part, part, result_recv_sem.at[m, s]).wait()

    edge_items = range(5)
    rest_items = range(5, len(items))
    prepare_edges()
    pl.semaphore_wait(barrier, ranks - 1 + (sections - 1) * sections)

    @pl.when(section == 0)
    def first_items():
        send_items(edge_items)

    for k in range(1, sections):
        stage_copy(0, k).wait()
        pair_copy(0, k).start()
    prepare_gains(section)

    @pl.when(section != 0)
    def other_items():
        prepare_rest()
        send_items(range(len(items)))

    for m in everyone:
        load_pair(m, 0)

    @pl.when(section != 0)
    def first_weights():
        pass_items(edge_items, 0)
        wait_items(edge_items, 0)
        prepare_gains(0)

    phase_norm(0, 0, 0)
    phase_edges(0, 0, 0)
    send_edges(0, 0, 0)
    for m in everyone[1:]:
        for k in range(1, sections):
            stage_copy(m, k).wait()
            pair_copy(m, k).start()

    @pl.when(section == 0)
    def second_items():
        prepare_rest()
        send_items(rest_items)

    for m in everyone[1:]:
        phase_norm(0, m, 0)
        phase_edges(0, m, 0)
    for other in range(1, sections):

        @pl.when(section != other)
        def relay_later():
            pass_items(range(len(items)), other)

    for m in everyone:
        for t in pieces[1:]:
            load_pair(m, t)
            phase_norm(0, m, t)
            phase_edges(0, m, t)
            send_edges(0, m, t)
        if m == 0:

            @pl.when(section != 0)
            def relay_first():
                pass_items(rest_items, 0)

        if m + 1 < own_count:
            send_edges(0, m + 1, 0)

    @pl.when(section != 0)
    def other_weights():
        wait_items(rest_items, 0)

    for m in everyone:
        for t in pieces:
            phase_gate(0, m, t)

    for layer in range(sections):
        last = layer == sections - 1
        order = pieces[::-1] if last else pieces
        for m in everyone:
            if layer > 0:
                wait_tri_sent(m)
            phase_triangle(layer % 2, m, order)
        if layer == 0:
            for other in range(1, sections):

                @pl.when(section != other)
                def later_weights():
                    wait_items(range(len(items)), other)
                    prepare_gains(other)

        for m in everyone:
            for t in order:
                wait_tri(m, t)
                phase_update(layer, m, t, last)
                wait_edges_sent(m, t)
                if last:
                    send_result(m, t)
                else:
                    phase_norm(layer + 1, m, t)
                    phase_edges(layer + 1, m, t)
                    send_edges((layer + 1) % 2, m, t)
        if not last:
            for m in everyone:
                for t in pieces:
                    phase_gate(layer + 1, m, t)
    for m in everyone:
        wait_tri_sent(m)
        for k in range(1, sections):
            pair_copy(m, k).wait_send()
    finish_items()
    finish_results()


def fused_device(pair_in, crop_mask, proj_weights, out_weights, up_weights, down_weights, norm_gains):
    sections = lax.axis_size("section")
    ranks = lax.axis_size("axial")
    micro_count, rows, width, channels = pair_in.shape
    own_count = micro_count // sections
    halves = half_count(pair_in)
    owners = ranks // halves
    per_group = channels // owners
    piece_rows = rows // sections
    sub_rows = 2 if piece_rows % 2 == 0 else 1
    steps = piece_rows // sub_rows
    lanes = sub_rows * width
    hidden = up_weights.shape[2]
    gains = norm_gains.shape[1]
    edge_kinds = proj_weights.shape[1]
    bf16, f32 = jnp.bfloat16, jnp.float32
    vmem = pl.BlockSpec(memory_space=pltpu.VMEM)
    hbm = pl.BlockSpec(memory_space=pltpu.HBM)
    dma = pltpu.SemaphoreType.DMA
    piece = (piece_rows, per_group, width)
    rows_shape = (own_count, sections, piece_rows, width, channels)
    wide_shape = (own_count, sections, steps, channels, lanes)
    tri_shape = (own_count, sections, owners) + piece
    return pl.pallas_call(
        functools.partial(fused_kernel, sections, ranks, halves, own_count, sub_rows),
        out_shape=pltpu.VMEM((own_count, rows, width, channels), bf16),
        in_specs=[hbm, vmem, pl.BlockSpec(memory_space=pltpu.SMEM)] + [hbm] * 5,
        out_specs=vmem,
        scratch_shapes=[
            pltpu.VMEM(rows_shape, bf16),
            pltpu.VMEM((own_count, sections - 1) + rows_shape[2:], bf16),
            pltpu.VMEM(wide_shape, f32),
            pltpu.VMEM(wide_shape, bf16),
            pltpu.VMEM(wide_shape, f32),
            pltpu.VMEM((own_count, sections, owners, 2) + piece, bf16),
            pltpu.VMEM((2, own_count, sections, ranks, 2) + piece, bf16),
            pltpu.VMEM(tri_shape, bf16),
            pltpu.VMEM(tri_shape, bf16),
            pltpu.VMEM((width // 128, owners * rows * per_group, 128), f32),
            pltpu.VMEM((width // 128, ranks * rows * per_group, 128), f32),
            pltpu.VMEM((width // 128, owners * rows * per_group, 128), f32),
            pltpu.VMEM(rows_shape, bf16),
            pltpu.VMEM(proj_weights.shape[1:], bf16),
            pltpu.VMEM(out_weights.shape[1:], bf16),
            pltpu.VMEM(up_weights.shape[1:], bf16),
            pltpu.VMEM(down_weights.shape[1:], bf16),
            pltpu.VMEM((sections,) + norm_gains.shape[1:], bf16),
            pltpu.VMEM((sections, edge_kinds, channels, channels), bf16),
            pltpu.VMEM((sections, channels, channels), bf16),
            pltpu.VMEM((sections, hidden, channels), bf16),
            pltpu.VMEM((sections, channels, hidden), bf16),
            pltpu.VMEM((sections, gains, channels, width), f32),
            dma((own_count, sections - 1)),
            dma((own_count, sections)),
            dma((own_count, sections)),
            dma((own_count, sections)),
            dma((2, own_count, sections)),
            dma((own_count, sections)),
            dma((own_count, sections)),
            dma((own_count, sections)),
            dma((own_count, sections)),
            dma((7,)),
            dma((9, sections)),
            dma((9, sections)),
            dma((9, sections)),
        ],
        compiler_params=pltpu.CompilerParams(
            collective_id=0, has_side_effects=True, vmem_limit_bytes=67043328 - 2 * own_count * rows * width * channels
        ),
    )(
        pair_in,
        crop_mask,
        crop_mask,
        proj_weights,
        out_weights,
        up_weights,
        down_weights,
        norm_gains,
    )


def half_count(pair_in):
    ranks = lax.axis_size("axial")
    return 2 if ranks % 2 == 0 and pair_in.shape[3] % (8 * ranks) else 1


def fits_fused(pair_in):
    rows, width, channels = pair_in.shape[1:]
    sections = lax.axis_size("section")
    ranks = lax.axis_size("axial")
    owners = ranks // half_count(pair_in)
    return (
        channels % (8 * owners) == 0
        and rows % sections == 0
        and width % 128 == 0
        and ranks % (2 * sections) == 0
    )


def per_device(pair_in, crop_mask, proj_weights, out_weights, up_weights, down_weights, norm_gains):
    if fits_fused(pair_in):
        return fused_device(
            pair_in, crop_mask, proj_weights, out_weights, up_weights, down_weights, norm_gains
        )
    section_index = lax.axis_index("section")
    section_count = lax.axis_size("section")
    micro_count = pair_in.shape[0]
    own_count = micro_count // section_count
    gathered = (
        lax.all_gather(proj_weights, "section", axis=0, tiled=True),
        lax.all_gather(out_weights, "section", axis=0, tiled=True),
        lax.all_gather(up_weights, "section", axis=0, tiled=True),
        lax.all_gather(down_weights, "section", axis=0, tiled=True),
        lax.all_gather(norm_gains, "section", axis=0, tiled=True),
    )
    own_pairs = lax.dynamic_slice_in_dim(pair_in, section_index * own_count, own_count, 0)
    own_masks = lax.dynamic_slice_in_dim(crop_mask, section_index * own_count, own_count, 0).astype(
        jnp.float32
    )
    outputs = []
    for member in range(own_count):
        current = own_pairs[member]
        for layer_index in range(section_count):
            current = evo_block(
                current,
                own_masks[member],
                gathered[0][layer_index],
                gathered[1][layer_index],
                gathered[2][layer_index],
                gathered[3][layer_index],
                gathered[4][layer_index],
            )
        outputs.append(current)
    return jnp.stack(outputs)


def solution(mesh):
    return jax.shard_map(
        per_device,
        mesh=mesh,
        in_specs=(
            P("groups", "axial", None, None),
            P("groups", None),
            P("section", None, None, None),
            P("section", None, None),
            P("section", None, None),
            P("section", None, None),
            P("section", None, None),
        ),
        out_specs=P(("groups", "section"), "axial", None, None),
        check_vma=False,
    )
```

```python
import functools

import jax
import jax.numpy as jnp
from jax import lax
from jax.experimental import pallas as pl
from jax.experimental.pallas import tpu as pltpu
from jax.sharding import PartitionSpec as P

epsilon = 1e-05


def normalize(values, axis_dim):
    center = values - jnp.mean(values, axis=axis_dim, keepdims=True)
    spread = jnp.mean(center * center, axis=axis_dim, keepdims=True)
    return center * lax.rsqrt(spread + epsilon)


def triangle(pieces):
    return jnp.einsum(
        "gcik,gcjk->gcij", pieces[0], pieces[1], preferred_element_type=jnp.float32
    ).astype(jnp.bfloat16)


def evo_block(current, mask_all, proj_mats, out_mat, up_mat, down_mat, gain_rows):
    row_count = current.shape[0]
    width = current.shape[1]
    channels = current.shape[2]
    group_count = lax.axis_size("axial")
    per_group = channels // group_count
    row_start = lax.axis_index("axial") * row_count
    mask_rows = lax.dynamic_slice_in_dim(mask_all, row_start, row_count)
    gain_vals = gain_rows.astype(jnp.float32)
    pair_f = current.astype(jnp.float32)
    normed = (normalize(pair_f, 2) * gain_vals[0]).astype(jnp.bfloat16)
    linear = jnp.einsum("rnd,edc->ecrn", normed, proj_mats[:4], preferred_element_type=jnp.float32)
    pair_mask = mask_rows[:, None] * mask_all[None, :]
    left_edge = (jax.nn.sigmoid(linear[1]) * linear[0] * pair_mask).astype(jnp.bfloat16)
    right_edge = (jax.nn.sigmoid(linear[3]) * linear[2] * pair_mask).astype(jnp.bfloat16)
    left_groups = left_edge.reshape(group_count, per_group, row_count, width)
    right_groups = right_edge.reshape(group_count, per_group, row_count, width)
    product = triangle(
        (
            lax.all_to_all(left_groups, "axial", split_axis=0, concat_axis=2, tiled=True),
            lax.all_to_all(right_groups, "axial", split_axis=0, concat_axis=2, tiled=True),
        )
    )
    restored = lax.all_to_all(product, "axial", split_axis=2, concat_axis=0, tiled=True).reshape(
        channels, row_count, width
    )
    tri_norm = (normalize(restored.astype(jnp.float32), 0) * gain_vals[1][:, None, None]).astype(
        jnp.bfloat16
    )
    update = jnp.einsum("crn,cd->rnd", tri_norm, out_mat, preferred_element_type=jnp.float32)
    gate_values = jax.nn.sigmoid(
        jnp.einsum("rnd,dc->rnc", normed, proj_mats[4], preferred_element_type=jnp.float32)
    )
    pair_mid = pair_f + gate_values * update
    trans_in = (normalize(pair_mid, 2) * gain_vals[2]).astype(jnp.bfloat16).reshape(-1, channels)
    hidden = jax.nn.relu(jnp.dot(trans_in, up_mat, preferred_element_type=jnp.float32)).astype(
        jnp.bfloat16
    )
    pair_new = pair_mid + jnp.dot(hidden, down_mat, preferred_element_type=jnp.float32).reshape(
        pair_mid.shape
    )
    return pair_new.astype(jnp.bfloat16)


MESH = pl.DeviceIdType.MESH


def sigmoid(values):
    return 0.5 * jnp.tanh(0.5 * values) + 0.5


def normalize_rows(values, gain):
    scale = 1.0 / values.shape[0]
    center = values - jnp.sum(values, axis=0, keepdims=True) * scale
    spread = jnp.sum(center * center, axis=0, keepdims=True) * scale
    return center * lax.rsqrt(spread + epsilon) * gain


def matmul(mat, values):
    return lax.dot_general(mat, values, (((1,), (0,)), ((), ())), preferred_element_type=jnp.float32)


def fused_kernel(
    sections,
    ranks,
    halves,
    own_count,
    sub_rows,
    pair_ref,
    mask_ref,
    mask_smem,
    proj_ref,
    out_ref,
    up_ref,
    down_ref,
    gain_ref,
    result_ref,
    pair_buf,
    pair_stage,
    z_buf,
    normed_buf,
    gate_buf,
    edge_send,
    edge_recv,
    tri_send,
    tri_recv,
    left_f,
    right_f,
    tri_f,
    result_buf,
    proj_raw,
    out_raw,
    up_raw,
    down_raw,
    gain_all,
    proj_t,
    out_t,
    up_t,
    down_t,
    gain_t,
    pair_stage_sem,
    pair_send_sem,
    pair_sem,
    edge_send_sem,
    edge_recv_sem,
    tri_send_sem,
    tri_recv_sem,
    result_send_sem,
    result_recv_sem,
    raw_sem,
    weight_send_sem,
    weight_pass_sem,
    weight_sem,
):
    section = lax.axis_index("section")
    axial = lax.axis_index("axial")
    span = ranks // sections
    group = axial // span
    place = lax.rem(axial, span)
    core = lax.rem(axial, 2)
    rank = section * span + place
    piece_rows, width, channels = pair_buf.shape[2:]
    rows = piece_rows * sections
    owners = ranks // halves
    per_group = channels // owners
    my_half = rank // owners
    my_owner = lax.rem(rank, owners)
    steps = piece_rows // sub_rows
    everyone = range(own_count)
    pieces = range(sections)

    def member(index):
        return {"section": index // span, "axial": group * span + lax.rem(index, span)}

    def part_of(t):
        return lax.rem(group + t, sections)

    def first_row(t, section_at, place_at):
        return (part_of(t) * span + place_at) * rows + section_at * piece_rows

    own_rows = pl.ds(section * piece_rows, piece_rows)

    barrier = pltpu.get_barrier_semaphore()
    for k in range(1, ranks):
        pl.semaphore_signal(
            barrier, inc=1, device_id=member(lax.rem(rank + k, ranks)), device_id_type=MESH
        )
    for k in range(1, sections):
        for j in range(sections):
            pl.semaphore_signal(
                barrier,
                inc=1,
                device_id={
                    "section": lax.rem(section + j, sections),
                    "axial": part_of(k) * span + place,
                },
                device_id_type=MESH,
            )

    def stage_copy(m, k):
        return pltpu.make_async_copy(
            pair_ref.at[part_of(k) * own_count + m, own_rows],
            pair_stage.at[m, k - 1],
            pair_stage_sem.at[m, k - 1],
        )

    for m in everyone:
        pltpu.make_async_copy(
            pair_ref.at[group * own_count + m, own_rows], pair_buf.at[m, 0], pair_sem.at[m, 0]
        ).start()
    for m in everyone:
        for k in range(1, sections):
            stage_copy(m, k).start()
    raw_copies = [
        pltpu.make_async_copy(source, target, raw_sem.at[index])
        for index, (source, target) in enumerate(
            (
                (gain_ref.at[0], gain_all.at[section]),
                (proj_ref.at[0, pl.ds(2, 2)], proj_raw.at[pl.ds(2, 2)]),
                (proj_ref.at[0, pl.ds(0, 2)], proj_raw.at[pl.ds(0, 2)]),
                (proj_ref.at[0, pl.ds(4, 1)], proj_raw.at[pl.ds(4, 1)]),
                (out_ref.at[0], out_raw),
                (up_ref.at[0], up_raw),
                (down_ref.at[0], down_raw),
            )
        )
    ]
    for copy in raw_copies:
        copy.start()

    items = (
        (1, lambda layer: gain_all.at[layer]),
        (1, lambda layer: proj_t.at[layer, 2]),
        (1, lambda layer: proj_t.at[layer, 3]),
        (1, lambda layer: proj_t.at[layer, 0]),
        (1, lambda layer: proj_t.at[layer, 1]),
        (1, lambda layer: proj_t.at[layer, 4]),
        (1, lambda layer: out_t.at[layer]),
        (0, lambda layer: up_t.at[layer]),
        (0, lambda layer: down_t.at[layer]),
    )

    def beyond(layer):
        return lax.rem(layer - section + sections, sections) - 1 if sections > 2 else 0

    def item_copy(a, k):
        view = items[a][1](section)
        return pltpu.make_async_remote_copy(
            src_ref=view,
            dst_ref=view,
            send_sem=weight_send_sem.at[a, k - 1],
            recv_sem=weight_sem.at[a, sections - 1 - k],
            device_id={"section": lax.rem(section + k, sections)},
            device_id_type=MESH,
        )

    def item_pass(a, layer):
        view = items[a][1](layer)
        return pltpu.make_async_remote_copy(
            src_ref=view,
            dst_ref=view,
            send_sem=weight_pass_sem.at[a, beyond(layer)],
            recv_sem=weight_sem.at[a, beyond(layer)],
            device_id={"axial": axial + 1 - 2 * core},
            device_id_type=MESH,
        )

    def send_items(chosen):
        for side in range(2):

            @pl.when(core == side)
            def start():
                for a in chosen:
                    if items[a][0] == side:
                        for k in range(1, sections):
                            item_copy(a, k).start()

    def wait_item(a, layer):
        view = items[a][1](layer)
        pltpu.make_async_copy(view, view, weight_sem.at[a, beyond(layer)]).wait()

    def pass_items(chosen, layer):
        for side in range(2):

            @pl.when(core == side)
            def give_on():
                for a in chosen:
                    if items[a][0] == side:
                        wait_item(a, layer)
                        item_pass(a, layer).start()

    def wait_items(chosen, layer):
        for side in range(2):

            @pl.when(core == side)
            def receive():
                for a in chosen:
                    if items[a][0] != side:
                        wait_item(a, layer)

    def finish_items():
        for side in range(2):

            @pl.when(core == side)
            def finish():
                for a, (owner, _) in enumerate(items):
                    if owner == side:
                        for k in range(1, sections):
                            item_copy(a, k).wait_send()
                        for k in range(1, sections):
                            item_pass(a, lax.rem(section + k, sections)).wait_send()

    def turned(values):
        return values.astype(jnp.float32).T.astype(jnp.bfloat16)

    def prepare_gains(layer):
        for index in range(gain_t.shape[1]):
            row = gain_all[layer, index : index + 1, :].astype(jnp.float32)
            gain_t[layer, index] = jnp.broadcast_to(row, (width, channels)).T

    def prepare_edges():
        raw_copies[0].wait()
        for pair in (1, 0):
            raw_copies[2 - pair].wait()
            for e in (2 * pair, 2 * pair + 1):
                proj_t[section, e] = turned(proj_raw[e])

    def prepare_rest():
        raw_copies[3].wait()
        proj_t[section, 4] = turned(proj_raw[4])
        for copy in raw_copies[4:]:
            copy.wait()
        out_t[section] = turned(out_raw[...])
        up_t[section] = turned(up_raw[...])
        down_t[section] = turned(down_raw[...])

    def wide_gain(layer, index):
        return jnp.concatenate([gain_t[layer, index]] * sub_rows, axis=1)

    def pair_copy(m, k):
        target = part_of(k)
        return pltpu.make_async_remote_copy(
            src_ref=pair_stage.at[m, k - 1],
            dst_ref=pair_buf.at[m, sections - k],
            send_sem=pair_send_sem.at[m, k - 1],
            recv_sem=pair_sem.at[m, sections - k],
            device_id={"axial": target * span + place},
            device_id_type=MESH,
        )

    def load_pair(m, t):
        pltpu.make_async_copy(pair_buf.at[m, t], pair_buf.at[m, t], pair_sem.at[m, t]).wait()
        for q in range(steps):
            for i in range(sub_rows):
                z_buf[m, t, q, :, i * width : (i + 1) * width] = (
                    pair_buf[m, t, q * sub_rows + i].astype(jnp.float32).T
                )

    def phase_norm(layer, m, t):
        for q in range(steps):
            normed_buf[m, t, q] = normalize_rows(z_buf[m, t, q], wide_gain(layer, 0)).astype(
                jnp.bfloat16
            )

    def phase_edges(layer, m, t):
        crop = group * own_count + m
        row_mask = mask_ref[pl.ds(crop, 1), :].astype(jnp.float32)
        start = first_row(t, section, place)
        for q in range(steps):
            values = normed_buf[m, t, q]
            masks = []
            for i in range(sub_rows):
                own = mask_smem[crop, start + q * sub_rows + i]
                masks.append(row_mask * own.astype(jnp.float32))
            pair_mask = jnp.concatenate(masks, axis=1)
            for side in (1, 0):
                value = matmul(proj_t[layer, 2 * side], values)
                gate = matmul(proj_t[layer, 2 * side + 1], values)
                edge = sigmoid(gate) * value * pair_mask
                for i in range(sub_rows):
                    part = edge[:, i * width : (i + 1) * width].reshape(owners, per_group, width)
                    edge_send[m, t, :, side, q * sub_rows + i] = part.astype(jnp.bfloat16)

    def phase_gate(layer, m, t):
        for q in range(steps):
            gate_buf[m, t, q] = sigmoid(matmul(proj_t[layer, 4], normed_buf[m, t, q]))

    def rank_at(half_step, index):
        if halves == 1:
            return index
        return lax.rem(my_half + half_step, halves) * owners + index

    def partner(k):
        if owners & (owners - 1):
            return lax.rem(my_owner + k, owners)
        index, unit = 0, 1
        while unit < owners:
            bit = lax.rem(my_owner // unit, 2)
            index += unit * (1 - bit if k // unit % 2 else bit)
            unit *= 2
        return index

    def edge_view(ref, half_step):
        return ref if half_step == 0 else ref.at[1]

    def edge_copy(slot, m, t, k):
        half_step = k // owners
        owner = partner(k % owners)
        return pltpu.make_async_remote_copy(
            src_ref=edge_view(edge_send.at[m, t, owner], half_step),
            dst_ref=edge_view(edge_recv.at[slot, m, t, rank], half_step),
            send_sem=edge_send_sem.at[m, t],
            recv_sem=edge_recv_sem.at[slot, m, t],
            device_id=member(rank_at(half_step, owner)),
            device_id_type=MESH,
        )

    def send_edges(slot, m, t):
        for k in range(ranks - 1, 0, -1):
            edge_copy(slot, m, t, k).start()
        pltpu.make_async_copy(
            edge_send.at[m, t, my_owner],
            edge_recv.at[slot, m, t, rank],
            edge_recv_sem.at[slot, m, t],
        ).start()

    def wait_edges_sent(m, t):
        left_over = (halves - 1) * owners
        sent = edge_recv.at[0, m, t, pl.ds(0, owners - 1 + left_over // 2)]
        pltpu.make_async_copy(sent, sent, edge_send_sem.at[m, t]).wait()

    def wait_edges(slot, m, t):
        left_over = (halves - 1) * owners
        got = edge_recv.at[slot, m, t, pl.ds(0, owners + left_over // 2)]
        pltpu.make_async_copy(got, got, edge_recv_sem.at[slot, m, t]).wait()

    def tri_copy(m, t, k):
        owner = partner(k)
        return pltpu.make_async_remote_copy(
            src_ref=tri_send.at[m, t, owner],
            dst_ref=tri_recv.at[m, t, my_owner],
            send_sem=tri_send_sem.at[m, t],
            recv_sem=tri_recv_sem.at[m, t],
            device_id=member(my_half * owners + owner),
            device_id_type=MESH,
        )

    def send_tri(m, t):
        for k in range(owners - 1, 0, -1):
            tri_copy(m, t, k).start()
        pltpu.make_async_copy(
            tri_send.at[m, t, my_owner], tri_recv.at[m, t, my_owner], tri_recv_sem.at[m, t]
        ).start()

    def wait_tri_sent(m):
        for t in pieces:
            sent = tri_recv.at[m, t, pl.ds(0, owners - 1)]
            pltpu.make_async_copy(sent, sent, tri_send_sem.at[m, t]).wait()

    def wait_tri(m, t):
        pltpu.make_async_copy(tri_recv.at[m, t], tri_recv.at[m, t], tri_recv_sem.at[m, t]).wait()

    def phase_triangle(slot, m, order):
        columns = [slice(w * 128, (w + 1) * 128) for w in range(width // 128)]
        piece_lines = piece_rows * per_group

        def spread(target, at, values):
            for w, lanes in enumerate(columns):
                target[w, pl.ds(at, piece_lines)] = (
                    values[:, :, lanes].astype(jnp.float32).reshape(piece_lines, 128)
                )

        def channel(source, c, count):
            lines = pl.ds(c, count, stride=per_group)
            return jnp.concatenate(
                [source[w, lines, :].astype(jnp.bfloat16) for w in range(len(columns))], axis=1
            )

        for t in pieces:
            wait_edges(slot, m, t)
            for half_step in range(halves):
                for index in range(owners):
                    g = rank_at(half_step, index)
                    start = first_row(t, g // span, g % span if halves == 1 else lax.rem(g, span))
                    spread(
                        right_f,
                        pl.multiple_of(start * per_group, 8),
                        edge_recv[slot, m, t, g, 1],
                    )
                    if half_step == 0:
                        at = index * rows + t * piece_rows
                        spread(left_f, at * per_group, edge_recv[slot, m, t, g, 0])
        for c in range(per_group):
            product = lax.dot_general(
                channel(left_f, c, owners * rows),
                channel(right_f, c, ranks * rows),
                (((1,), (1,)), ((), ())),
                preferred_element_type=jnp.float32,
            )
            for w, lanes in enumerate(columns):
                tri_f[w, pl.ds(c, owners * rows, stride=per_group), :] = product[:, lanes]
        for t in order:
            for g in range(owners):
                at = (g * rows + t * piece_rows) * per_group
                for w, lanes in enumerate(columns):
                    part = tri_f[w, at : at + piece_lines].reshape(piece_rows, per_group, 128)
                    tri_send[m, t, g, :, :, lanes] = part.astype(jnp.bfloat16)
            send_tri(m, t)

    def phase_update(layer, m, t, last):
        span_q = range(steps)

        def tri_at(q):
            parts = []
            for i in range(sub_rows):
                part = tri_recv[m, t, :, q * sub_rows + i].astype(jnp.float32)
                parts.append(part.reshape(channels, width))
            return jnp.concatenate(parts, axis=1)

        gain_tri, gain_in = wide_gain(layer, 1), wide_gain(layer, 2)
        tri_norm = [normalize_rows(tri_at(q), gain_tri).astype(jnp.bfloat16) for q in span_q]
        update = [matmul(out_t[layer], tri_norm[q]) for q in span_q]
        mid = [z_buf[m, t, q] + gate_buf[m, t, q] * update[q] for q in span_q]
        trans_in = [normalize_rows(mid[q], gain_in).astype(jnp.bfloat16) for q in span_q]
        hidden = [
            jnp.maximum(matmul(up_t[layer], trans_in[q]), 0.0).astype(jnp.bfloat16) for q in span_q
        ]
        fresh = [mid[q] + matmul(down_t[layer], hidden[q]) for q in span_q]
        for q in span_q:
            if last:
                for i in range(sub_rows):
                    part = fresh[q][:, i * width : (i + 1) * width]
                    result_buf[m, t, q * sub_rows + i] = part.T.astype(jnp.bfloat16)
            else:
                z_buf[m, t, q] = fresh[q].astype(jnp.bfloat16).astype(jnp.float32)

    def result_copy(m, t):
        return pltpu.make_async_remote_copy(
            src_ref=result_buf.at[m, t],
            dst_ref=result_ref.at[m, own_rows],
            send_sem=result_send_sem.at[m, t],
            recv_sem=result_recv_sem.at[m, section],
            device_id={"section": group, "axial": part_of(t) * span + place},
            device_id_type=MESH,
        )

    def send_result(m, t):
        if t > 0:
            result_copy(m, t).start()
            return

        @pl.when(section == group)
        def keep():
            pltpu.make_async_copy(
                result_buf.at[m, t], result_ref.at[m, own_rows], result_recv_sem.at[m, section]
            ).start()

        @pl.when(section != group)
        def give():
            result_copy(m, t).start()

    def finish_results():
        for m in everyone:
            for t in pieces:
                if t > 0:
                    result_copy(m, t).wait_send()
                else:

                    @pl.when(section != group)
                    def given():
                        result_copy(m, t).wait_send()

            for s in range(sections):
                part = result_ref.at[m, pl.ds(s * piece_rows, piece_rows)]
                pltpu.make_async_copy(part, part, result_recv_sem.at[m, s]).wait()

    edge_items = range(5)
    rest_items = range(5, len(items))
    prepare_edges()
    pl.semaphore_wait(barrier, ranks - 1 + (sections - 1) * sections)

    @pl.when(section == 0)
    def first_items():
        send_items(edge_items)

    for k in range(1, sections):
        stage_copy(0, k).wait()
        pair_copy(0, k).start()
    prepare_gains(section)

    @pl.when(section != 0)
    def other_items():
        prepare_rest()
        send_items(range(len(items)))

    for m in everyone:
        load_pair(m, 0)

    @pl.when(section != 0)
    def first_weights():
        pass_items(edge_items, 0)
        wait_items(edge_items, 0)
        prepare_gains(0)

    phase_norm(0, 0, 0)
    phase_edges(0, 0, 0)
    send_edges(0, 0, 0)
    for m in everyone[1:]:
        for k in range(1, sections):
            stage_copy(m, k).wait()
            pair_copy(m, k).start()

    @pl.when(section == 0)
    def second_items():
        prepare_rest()
        send_items(rest_items)

    for m in everyone[1:]:
        phase_norm(0, m, 0)
        phase_edges(0, m, 0)
    for other in range(1, sections):

        @pl.when(section != other)
        def relay_later():
            pass_items(range(len(items)), other)

    for m in everyone:
        for t in pieces[1:]:
            load_pair(m, t)
            phase_norm(0, m, t)
            phase_edges(0, m, t)
            send_edges(0, m, t)
        if m == 0:

            @pl.when(section != 0)
            def relay_first():
                pass_items(rest_items, 0)

        if m + 1 < own_count:
            send_edges(0, m + 1, 0)

    @pl.when(section != 0)
    def other_weights():
        wait_items(rest_items, 0)

    for m in everyone:
        for t in pieces:
            phase_gate(0, m, t)

    for layer in range(sections):
        last = layer == sections - 1
        order = pieces[::-1] if last else pieces
        for m in everyone:
            if layer > 0:
                wait_tri_sent(m)
            phase_triangle(layer % 2, m, order)
        if layer == 0:
            for other in range(1, sections):

                @pl.when(section != other)
                def later_weights():
                    wait_items(range(len(items)), other)
                    prepare_gains(other)

        for m in everyone:
            for t in order:
                wait_tri(m, t)
                phase_update(layer, m, t, last)
                wait_edges_sent(m, t)
                if last:
                    send_result(m, t)
                else:
                    phase_norm(layer + 1, m, t)
                    phase_edges(layer + 1, m, t)
                    send_edges((layer + 1) % 2, m, t)
        if not last:
            for m in everyone:
                for t in pieces:
                    phase_gate(layer + 1, m, t)
    for m in everyone:
        wait_tri_sent(m)
        for k in range(1, sections):
            pair_copy(m, k).wait_send()
    finish_items()
    finish_results()


def fused_device(pair_in, crop_mask, proj_weights, out_weights, up_weights, down_weights, norm_gains):
    sections = lax.axis_size("section")
    ranks = lax.axis_size("axial")
    micro_count, rows, width, channels = pair_in.shape
    own_count = micro_count // sections
    halves = half_count(pair_in)
    owners = ranks // halves
    per_group = channels // owners
    piece_rows = rows // sections
    sub_rows = 2 if piece_rows % 2 == 0 else 1
    steps = piece_rows // sub_rows
    lanes = sub_rows * width
    hidden = up_weights.shape[2]
    gains = norm_gains.shape[1]
    edge_kinds = proj_weights.shape[1]
    bf16, f32 = jnp.bfloat16, jnp.float32
    vmem = pl.BlockSpec(memory_space=pltpu.VMEM)
    hbm = pl.BlockSpec(memory_space=pltpu.HBM)
    dma = pltpu.SemaphoreType.DMA
    piece = (piece_rows, per_group, width)
    rows_shape = (own_count, sections, piece_rows, width, channels)
    wide_shape = (own_count, sections, steps, channels, lanes)
    tri_shape = (own_count, sections, owners) + piece
    return pl.pallas_call(
        functools.partial(fused_kernel, sections, ranks, halves, own_count, sub_rows),
        out_shape=pltpu.VMEM((own_count, rows, width, channels), bf16),
        in_specs=[hbm, vmem, pl.BlockSpec(memory_space=pltpu.SMEM)] + [hbm] * 5,
        out_specs=vmem,
        scratch_shapes=[
            pltpu.VMEM(rows_shape, bf16),
            pltpu.VMEM((own_count, sections - 1) + rows_shape[2:], bf16),
            pltpu.VMEM(wide_shape, f32),
            pltpu.VMEM(wide_shape, bf16),
            pltpu.VMEM(wide_shape, f32),
            pltpu.VMEM((own_count, sections, owners, 2) + piece, bf16),
            pltpu.VMEM((2, own_count, sections, ranks, 2) + piece, bf16),
            pltpu.VMEM(tri_shape, bf16),
            pltpu.VMEM(tri_shape, bf16),
            pltpu.VMEM((width // 128, owners * rows * per_group, 128), f32),
            pltpu.VMEM((width // 128, ranks * rows * per_group, 128), f32),
            pltpu.VMEM((width // 128, owners * rows * per_group, 128), f32),
            pltpu.VMEM(rows_shape, bf16),
            pltpu.VMEM(proj_weights.shape[1:], bf16),
            pltpu.VMEM(out_weights.shape[1:], bf16),
            pltpu.VMEM(up_weights.shape[1:], bf16),
            pltpu.VMEM(down_weights.shape[1:], bf16),
            pltpu.VMEM((sections,) + norm_gains.shape[1:], bf16),
            pltpu.VMEM((sections, edge_kinds, channels, channels), bf16),
            pltpu.VMEM((sections, channels, channels), bf16),
            pltpu.VMEM((sections, hidden, channels), bf16),
            pltpu.VMEM((sections, channels, hidden), bf16),
            pltpu.VMEM((sections, gains, channels, width), f32),
            dma((own_count, sections - 1)),
            dma((own_count, sections - 1)),
            dma((own_count, sections)),
            dma((own_count, sections)),
            dma((2, own_count, sections)),
            dma((own_count, sections)),
            dma((own_count, sections)),
            dma((own_count, sections)),
            dma((own_count, sections)),
            dma((7,)),
            dma((9, sections - 1)),
            dma((9, sections - 1)),
            dma((9, sections - 1)),
        ],
        compiler_params=pltpu.CompilerParams(
            collective_id=0, has_side_effects=True, vmem_limit_bytes=67043328 - 2 * own_count * rows * width * channels
        ),
    )(
        pair_in,
        crop_mask,
        crop_mask,
        proj_weights,
        out_weights,
        up_weights,
        down_weights,
        norm_gains,
    )


def half_count(pair_in):
    ranks = lax.axis_size("axial")
    return 2 if ranks % 2 == 0 and pair_in.shape[3] % (8 * ranks) else 1


def fits_fused(pair_in):
    rows, width, channels = pair_in.shape[1:]
    sections = lax.axis_size("section")
    ranks = lax.axis_size("axial")
    owners = ranks // half_count(pair_in)
    return (
        channels % (8 * owners) == 0
        and rows % sections == 0
        and width % 128 == 0
        and ranks % (2 * sections) == 0
    )


def per_device(pair_in, crop_mask, proj_weights, out_weights, up_weights, down_weights, norm_gains):
    if fits_fused(pair_in):
        return fused_device(
            pair_in, crop_mask, proj_weights, out_weights, up_weights, down_weights, norm_gains
        )
    section_index = lax.axis_index("section")
    section_count = lax.axis_size("section")
    micro_count = pair_in.shape[0]
    own_count = micro_count // section_count
    gathered = (
        lax.all_gather(proj_weights, "section", axis=0, tiled=True),
        lax.all_gather(out_weights, "section", axis=0, tiled=True),
        lax.all_gather(up_weights, "section", axis=0, tiled=True),
        lax.all_gather(down_weights, "section", axis=0, tiled=True),
        lax.all_gather(norm_gains, "section", axis=0, tiled=True),
    )
    own_pairs = lax.dynamic_slice_in_dim(pair_in, section_index * own_count, own_count, 0)
    own_masks = lax.dynamic_slice_in_dim(crop_mask, section_index * own_count, own_count, 0).astype(
        jnp.float32
    )
    outputs = []
    for member in range(own_count):
        current = own_pairs[member]
        for layer_index in range(section_count):
            current = evo_block(
                current,
                own_masks[member],
                gathered[0][layer_index],
                gathered[1][layer_index],
                gathered[2][layer_index],
                gathered[3][layer_index],
                gathered[4][layer_index],
            )
        outputs.append(current)
    return jnp.stack(outputs)


def solution(mesh):
    return jax.shard_map(
        per_device,
        mesh=mesh,
        in_specs=(
            P("groups", "axial", None, None),
            P("groups", None),
            P("section", None, None, None),
            P("section", None, None),
            P("section", None, None),
            P("section", None, None),
            P("section", None, None),
        ),
        out_specs=P(("groups", "section"), "axial", None, None),
        check_vma=False,
    )
```
